32 devices in a mesh: replica: 8 (over y, x, core), model: 4 (over z).
Axes of the slice: x: 2, y: 2, z: 4, core: 2. Of those that a mesh axis runs over, the one named last changes fastest.
Arguments:
- slope_gate: float32 [8, 2048, 6144], P('replica', None, 'model'), may hold values from -0.875 to 0.875
- slope_up: float32 [8, 2048, 6144], P('replica', None, 'model'), may hold values from -0.875 to 0.875
- slope_down: float32 [8, 6144, 2048], P('replica', 'model'), may hold values from -0.875 to 0.875
- slope_norm: float32 [8, 2048], P('replica'), may hold values from -8 to 8
- param_gate: float32 [2048, 6144], P('replica', 'model'), may hold values from -0.1875 to 0.1875
- param_up: float32 [2048, 6144], P('replica', 'model'), may hold values from -0.1875 to 0.1875
- param_down: float32 [6144, 2048], P('model', 'replica'), may hold values from -0.109375 to 0.109375
- param_norm: float32 [2048], P('replica'), may hold values from 0.25 to 1.75
Outputs:
- half_gate: bfloat16 [2048, 6144], P(None, 'model')
- half_up: bfloat16 [2048, 6144], P(None, 'model')
- half_down: bfloat16 [6144, 2048], P('model')
- half_norm: bfloat16 [2048], replicated
- next_gate: float32 [2048, 6144], P('replica', 'model')
- next_up: float32 [2048, 6144], P('replica', 'model')
- next_down: float32 [6144, 2048], P('model', 'replica')
- next_norm: float32 [2048], P('replica')
The draws below stay inside these ranges and needn't reach their ends.
All inputs are finite; a program needn't handle non-finite values.
Results may differ from the reference program's by a relative error of at most 0.0004.
Values may be sent and summed in bfloat16 or wider, within the bound.
A program may use at most 128 MiB of HBM per device.

```python
import jax
import jax.numpy as jnp
from jax import lax

WIDTH = 2048
INNER = 6144
REPLICAS = 8


def strengthened(values, stream_key, source, target, shards_of, factor):
    owner, partner = [(jnp.arange(values.shape[dim]) // (values.shape[dim] // shards_of)).reshape([-1 if axis == dim else 1 for axis in range(values.ndim)]) for dim in (source, target)]
    chosen = jax.random.permutation(stream_key, shards_of)[partner]
    strong = (owner == chosen) | (owner == (partner + shards_of // 2) % shards_of)
    return jnp.where(strong, factor * values, values)


def levels(stream_key, shape, cuts, low, top_value):
    def one(dim, parts):
        draws = jax.random.uniform(jax.random.fold_in(jax.random.fold_in(stream_key, 6), dim), (parts,), jnp.float32, low / len(cuts), top_value / len(cuts))
        return jnp.repeat(jnp.exp(draws), shape[dim] // parts).reshape((-1,) + (1,) * (len(shape) - dim - 1))

    factor_of = one(*cuts[0])
    for cut in cuts[1:]:
        factor_of = factor_of * one(*cut)
    return factor_of


def noise_with(key, dims, width, most, shards, heavy, dtype=jnp.bfloat16):
    drawn = width * jax.random.normal(key, dims, jnp.float32)
    if shards:
        drawn = drawn * levels(key, dims, shards, -0.22, 0.18)
    return jnp.clip(strengthened(drawn, jax.random.fold_in(key, 3), *heavy), -most, most).astype(dtype)


def setup_inputs(seed: int = 0) -> dict:
    arg_keys = jax.random.split(jax.random.key(seed), 9)
    return {
        "slope_gate": noise_with(arg_keys[0], (REPLICAS, WIDTH, INNER), 0.1, 0.875, ((0, 8), (2, 4)), (0, 1, 8, 2.0), jnp.float32),
        "slope_up": noise_with(arg_keys[1], (REPLICAS, WIDTH, INNER), 0.1, 0.875, ((0, 8), (2, 4)), (0, 1, 8, 2.0), jnp.float32),
        "slope_down": noise_with(arg_keys[2], (REPLICAS, INNER, WIDTH), 0.1, 0.875, ((0, 8), (1, 4)), (0, 2, 8, 2.0), jnp.float32),
        "slope_norm": noise_with(arg_keys[3], (REPLICAS, WIDTH), 1.0, 8.0, ((0, 8),), (0, 1, 8, 2.0), jnp.float32),
        "param_gate": noise_with(arg_keys[4], (WIDTH, INNER), WIDTH ** -0.5, 0.1875, ((0, 8), (1, 4)), (1, 0, 8, 2.0), jnp.float32),
        "param_up": noise_with(arg_keys[5], (WIDTH, INNER), WIDTH ** -0.5, 0.1875, ((0, 8), (1, 4)), (1, 0, 8, 2.0), jnp.float32),
        "param_down": noise_with(arg_keys[6], (INNER, WIDTH), INNER ** -0.5, 0.109375, ((0, 4), (1, 8)), (0, 1, 8, 2.0), jnp.float32),
        "param_norm": jnp.clip(1.0 + 0.15 * jax.random.normal(arg_keys[7], (WIDTH,), jnp.float32), 0.25, 1.75),
    }


learn_rate = 0.5

def reference(slope_gate, slope_up, slope_down, slope_norm, param_gate, param_up, param_down, param_norm):
    mean_gate = lax.optimization_barrier(jnp.sum(slope_gate.astype(jnp.float32), axis=0)) * REPLICAS ** (-0.5)
    mean_up = lax.optimization_barrier(jnp.sum(slope_up.astype(jnp.float32), axis=0)) * REPLICAS ** (-0.5)
    mean_down = lax.optimization_barrier(jnp.sum(slope_down.astype(jnp.float32), axis=0)) * REPLICAS ** (-0.5)
    mean_norm = lax.optimization_barrier(jnp.sum(slope_norm.astype(jnp.float32), axis=0)) * REPLICAS ** (-0.5)
    ratio_gate = jnp.sqrt(lax.optimization_barrier(jnp.sum(param_gate * param_gate, axis=1, keepdims=True))) * lax.rsqrt(lax.optimization_barrier(jnp.sum(mean_gate * mean_gate, axis=1, keepdims=True)) + 1e-06)
    mean_gate = mean_gate * ratio_gate
    ratio_up = jnp.sqrt(lax.optimization_barrier(jnp.sum(param_up * param_up, axis=1, keepdims=True))) * lax.rsqrt(lax.optimization_barrier(jnp.sum(mean_up * mean_up, axis=1, keepdims=True)) + 1e-06)
    mean_up = mean_up * ratio_up
    ratio_down = jnp.sqrt(lax.optimization_barrier(jnp.sum(param_down * param_down, axis=0, keepdims=True))) * lax.rsqrt(lax.optimization_barrier(jnp.sum(mean_down * mean_down, axis=0, keepdims=True)) + 1e-06)
    mean_down = mean_down * ratio_down
    next_gate = param_gate - learn_rate * mean_gate
    next_up = param_up - learn_rate * mean_up
    next_down = param_down - learn_rate * mean_down
    next_norm = param_norm - learn_rate * mean_norm
    half_gate = next_gate.astype(jnp.bfloat16)
    half_up = next_up.astype(jnp.bfloat16)
    half_down = next_down.astype(jnp.bfloat16)
    half_norm = next_norm.astype(jnp.bfloat16)
    return (half_gate, half_up, half_down, half_norm, next_gate, next_up, next_down, next_norm)
```

```python
import functools

import jax
import jax.numpy as jnp
from jax import lax
from jax.experimental import pallas as pl
from jax.experimental.pallas import tpu as pltpu
from jax.sharding import PartitionSpec as P

learn_rate = 0.5
eps = 1e-06
MESH = pl.DeviceIdType.MESH
f32, bf16 = jnp.float32, jnp.bfloat16
PIECES = 2
SLOTS = 4
OCTAVES = 252.0
LOW = -125.0
LN2 = 0.6931471805599453


def tile_rows(columns, most=24576):
    return 16 * max(1, most // (16 * columns))


def tiles(shape):
    return [
        (slice(r, r + 16), slice(c, c + 128))
        for r in range(0, shape[0], 16)
        for c in range(0, shape[1], 128)
    ]


def largest(t):
    top = None
    for r in range(0, t.shape[0], 8):
        for c in range(0, t.shape[1], 128):
            part = jnp.abs(t[r : r + 8, c : c + 128])
            top = part if top is None else jnp.maximum(top, part)
    return top


def doubled(t):
    return jnp.concatenate([t, t], axis=0)


def encode(t, scale):
    power = jnp.exp2(jnp.abs(t) * scale + LOW)
    return jnp.where(t < 0, -power, power).astype(bf16)


def decode(t, slope, base):
    t = t.astype(f32)
    size = jnp.log(jnp.abs(t)) * slope + base
    return jnp.where(t < 0, -size, size)


def encoder(top):
    return doubled(OCTAVES / top)


def decoder(top):
    return doubled(top * (1.0 / (OCTAVES * LN2))), doubled(top * (-LOW / OCTAVES))


def decode_block(ref, start, shape, code):
    rows = []
    for r in range(0, shape[0], 16):
        at = pl.ds(pl.multiple_of(start + r, 16), 16)
        rows.append(
            jnp.concatenate(
                [decode(ref[at, c : c + 128], *code) for c in range(0, shape[1], 128)], axis=1
            )
        )
    return jnp.concatenate(rows, axis=0) if len(rows) > 1 else rows[0]


def kernel(
    replicas, models,
    g_ref, u_ref, d_ref, nv_ref, pg_ref, pu_ref, pd_ref,
    hg_ref, hu_ref, hd_ref, ng_ref, nu_ref, nd_ref, hn_ref, nn_ref,
    pr_g, pr_u, pr_d, c1_g, c1_u, c1_d, r1_g, r1_u, r1_d,
    c2_g, c2_u, c2_d, r2_g, r2_u, r2_d, mn_g, mn_u, mn_d,
    ow_w, ow_d, hb_g, hb_u, hb_d, top1, got1, top2, got2,
    nrm_w, nrm_d, zs, zr_w, zr_d, ratios, nr, whole,
    ow_sem, pr_send, pr_recv, s1_send, s1_recv, s2_send, s2_recv,
    t1_send, t1_recv, t2_send, t2_recv,
    z_send, z_recv, n_send, n_recv, ag_send, ag_recv, loc_sem, next_sem,
):
    me = lax.axis_index("replica")
    z = lax.axis_index("model")
    k = lax.rem(me, 2)
    x = lax.rem(me // 2, 2)
    y = me // 4
    partner = me + 1 - 2 * k
    xn = me + 2 - 4 * x
    yn = me + 4 - 8 * y
    rate = replicas ** (-0.5)

    slopes = (g_ref, u_ref, d_ref)
    params = (pg_ref, pu_ref, pd_ref)
    halves = (hg_ref, hu_ref, hd_ref)
    nexts = (ng_ref, nu_ref, nd_ref)
    pr, mn = (pr_g, pr_u, pr_d), (mn_g, mn_u, mn_d)
    c1, r1 = (c1_g, c1_u, c1_d), (r1_g, r1_u, r1_d)
    c2, r2 = (c2_g, c2_u, c2_d), (r2_g, r2_u, r2_d)
    hb = (hb_g, hb_u, hb_d)
    units = 2 * PIECES
    side = pd_ref.shape[1]
    bands = pg_ref.shape[0] // 128

    others = [lax.rem(me + d, replicas) for d in range(1, replicas)]
    layers = [lax.rem(z + d, models) for d in range(1, models)]
    barrier = pltpu.get_barrier_semaphore()
    for other in others:
        pl.semaphore_signal(barrier, inc=1, device_id=(other, z), device_id_type=MESH)
    for layer in layers:
        pl.semaphore_signal(barrier, inc=1, device_id=(me, layer), device_id_type=MESH)
    pl.semaphore_wait(barrier, replicas - 1 + models - 1)

    sent = []

    def remote(src, dst, send_sem, recv_sem, to):
        return pltpu.make_async_remote_copy(
            src_ref=src, dst_ref=dst, send_sem=send_sem, recv_sem=recv_sem,
            device_id=to, device_id_type=MESH,
        )

    def start(copy):
        copy.start()
        sent.append(copy)

    def height(m):
        return mn[m].shape[0] // units

    def views(m, u, core):
        rows = pl.ds(u * height(m), height(m))
        if m < 2:
            return [(slopes[m].at[:, :, core, rows, :], None)]
        return [
            (
                slopes[m].at[
                    rows, pl.ds(pl.multiple_of((2 * c + core) * side, side), side)
                ],
                (c // 2, c % 2),
            )
            for c in range(4)
        ]

    def own_copies(m, u):
        ow = ow_w if m < 2 else ow_d
        slot = (m * units + order[u]) % SLOTS
        copies = []
        for n, (src, where) in enumerate(views(m, u, k)):
            dst = ow.at[slot] if where is None else ow.at[slot, where[0], where[1]]
            copies.append(pltpu.make_async_copy(src, dst, ow_sem.at[m, u, n]))
        return copies

    def pair_copies(m, u):
        copies = []
        for n, (src, where) in enumerate(views(m, u, 1 - k)):
            dst = pr[m].at[u] if where is None else pr[m].at[u, where[0], where[1]]
            copies.append(
                remote(src, dst, pr_send.at[m, u, n], pr_recv.at[m, u, n], (partner, z))
            )
        return copies

    sequence = [h * PIECES + j for j in range(PIECES) for h in range(2)]
    order = {u: n for n, u in enumerate(sequence)}
    jobs = [(m, u) for m in range(3) for u in sequence]

    for m, u in jobs[:SLOTS]:
        for copy in own_copies(m, u):
            copy.start()
    for m, u in jobs:
        for copy in pair_copies(m, u):
            start(copy)
    nr[me] = nv_ref[...]
    for n, other in enumerate(others):
        start(remote(nv_ref, nr.at[me], n_send.at[n], n_recv.at[me], (other, z)))

    def first_copies(m, u):
        to = (xn if u < PIECES else yn, z)
        return [
            remote(top1.at[m, u], got1.at[m, u], t1_send.at[m, u], t1_recv.at[m, u], to),
            remote(c1[m].at[u], r1[m].at[u], s1_send.at[m, u], s1_recv.at[m, u], to),
        ]

    def second_copies(m, u):
        to = (yn if u < PIECES else xn, z)
        return [
            remote(top2.at[m, u], got2.at[m, u], t2_send.at[m, u], t2_recv.at[m, u], to),
            remote(c2[m].at[u], r2[m].at[u], s2_send.at[m, u], s2_recv.at[m, u], to),
        ]

    def sweep(m, body, carry=None):
        step = tile_rows(mn[m].shape[1])
        trips = height(m) // step
        if carry is None:
            pl.loop(0, trips)(lambda i: body(i * step, step))
            return None
        return lax.fori_loop(0, trips, lambda i, c: body(i * step, step, c), carry)

    def code_out(m, values, dst, top):
        scale = encoder(top)

        def body(at, step):
            for r in range(0, step, 16):
                rows = pl.ds(pl.multiple_of(at + r, 16), 16)
                for c in range(0, mn[m].shape[1], 128):
                    dst[rows, c : c + 128] = encode(values[rows, c : c + 128], scale)

        sweep(m, body)

    blank = jnp.full((8, 128), 1e-30, f32)

    def stage_1(n):
        m, u = jobs[n]
        ow = ow_w if m < 2 else ow_d
        slot = n % SLOTS
        for copy in own_copies(m, u):
            copy.wait()
        for copy in pair_copies(m, u):
            copy.wait_recv()

        def add(at, step, a, b):
            rows = pl.ds(pl.multiple_of(at, 16), step)
            both = pr[m][u, a, b, rows, :] + ow[slot, a, b, rows, :]
            pr[m][u, a, b, rows, :] = both
            return both

        for j in range(2):
            a, b = (j, 1 - x) if u < PIECES else (1 - y, j)
            top = sweep(
                m, lambda at, step, c: jnp.maximum(c, largest(add(at, step, a, b))), blank
            )
            top1[m, u, j] = top
            code_out(m, pr[m].at[u, a, b], c1[m].at[u, j], top)
        for copy in first_copies(m, u):
            start(copy)
        for j in range(2):
            a, b = (j, x) if u < PIECES else (y, j)

            def keep(at, step):
                add(at, step, a, b)

            sweep(m, keep)
        if n + SLOTS < len(jobs):
            for copy in own_copies(*jobs[n + SLOTS]):
                copy.start()

    def stage_2(n):
        m, u = jobs[n]
        for copy in first_copies(m, u):
            copy.wait_recv()
        j, a, b = (1 - y, 1 - y, x) if u < PIECES else (1 - x, y, 1 - x)
        code = decoder(got1[m, u, j])
        columns = mn[m].shape[1]

        def body(at, step, c):
            rows = pl.ds(pl.multiple_of(at, 16), step)
            both = pr[m][u, a, b, rows, :] + decode_block(
                r1[m].at[u, j], at, (step, columns), code
            )
            pr[m][u, a, b, rows, :] = both
            return jnp.maximum(c, largest(both))

        top = sweep(m, body, blank)
        top2[m, u] = top
        code_out(m, pr[m].at[u, a, b], c2[m].at[u], top)
        for copy in second_copies(m, u):
            start(copy)

    def lanes(t):
        total = t[:, :128]
        for c in range(1, t.shape[1] // 128):
            total = total + t[:, c * 128 : (c + 1) * 128]
        return total

    def sublanes(t):
        total = t[:8]
        for c in range(1, t.shape[0] // 8):
            total = total + t[c * 8 : (c + 1) * 8]
        return total

    def stage_3(n):
        m, u = jobs[n]
        for copy in second_copies(m, u):
            copy.wait_recv()
        columns = mn[m].shape[1]
        near = decoder(got1[m, u, y if u < PIECES else x])
        far = decoder(got2[m, u])
        if m == 2 and u == sequence[0]:
            nrm_d[...] = jnp.zeros_like(nrm_d)

        def body(at, step):
            rows = pl.ds(pl.multiple_of(at, 16), step)
            here = pl.ds(pl.multiple_of(u * height(m) + at, 16), step)
            kept = r1[m].at[u, y if u < PIECES else x]
            mean = pr[m][u, y, x, rows, :] + decode_block(kept, at, (step, columns), near)
            mean = (mean + decode_block(r2[m].at[u], at, (step, columns), far)) * rate
            param = params[m][here, :]
            mn[m][here, :] = mean
            if m < 2:
                nrm_w[m, 0, here, :] = lanes(param * param)
                nrm_w[m, 1, here, :] = lanes(mean * mean)
            else:
                nrm_d[0] = nrm_d[0] + sublanes(param * param)
                nrm_d[1] = nrm_d[1] + sublanes(mean * mean)

        sweep(m, body)

    def size_copies(m):
        src = zs.at[m] if m < 2 else nrm_d
        return [
            remote(
                src, zr_w.at[m, n] if m < 2 else zr_d.at[n],
                z_send.at[m, n], z_recv.at[m, n], (me, layer),
            )
            for n, layer in enumerate(layers)
        ]

    def send_sizes(m):
        if m < 2:
            for q in range(2):
                for b in range(bands):
                    block = nrm_w[m, q, b * 128 : (b + 1) * 128, :]
                    row = q * bands + b
                    zs[m, row : row + 1, :] = jnp.sum(block.T, axis=0, keepdims=True)
        for copy in size_copies(m):
            start(copy)

    def piece(m, chip, core, h):
        ref = halves[m]
        tall = mn[m].shape[0] // 2
        if m < 2:
            at = pl.multiple_of((2 * chip + core) * mn[0].shape[0], mn[0].shape[0])
            return ref.at[pl.ds(pl.multiple_of(at + h * tall, tall), tall), :]
        at = pl.multiple_of((2 * chip + core) * side, side)
        return ref.at[pl.ds(h * tall, tall), pl.ds(at, side)]

    chip, chip_x, chip_y, chip_d = me // 2, xn // 2, yn // 2, 3 - me // 2

    def gather(m, h, way, src, at, to):
        return remote(src, at, ag_send.at[m, h, way], ag_recv.at[m, h, way], (to, z))

    def await_piece(m, h, way, chip_from, core):
        at = piece(m, chip_from, core, h)
        gather(m, h, way, at, at, partner).wait_recv()
        return at

    local = []

    def update(m):
        for copy in size_copies(m):
            copy.wait_recv()
        if m == 2:
            both = nrm_d[...]
            for n in range(models - 1):
                both = both + zr_d[n]
            own = jnp.sum(both[0], axis=0, keepdims=True)
            size = jnp.sum(both[1], axis=0, keepdims=True)
            ratio_d = jnp.sqrt(own) * lax.rsqrt(size + eps)
        else:
            both = zs[m]
            for n in range(models - 1):
                both = both + zr_w[m, n]
            ratio = jnp.sqrt(both[:bands]) * lax.rsqrt(both[bands : 2 * bands] + eps)
            for b in range(bands):
                ratios[b * 128 : (b + 1) * 128, :] = jnp.broadcast_to(
                    ratio[b : b + 1], (128, 128)
                ).T
        columns = mn[m].shape[1]
        step = tile_rows(columns)
        tall = mn[m].shape[0] // 2
        for h in range(2):

            @pl.loop(0, tall // step)
            def _(i):
                rows = pl.ds(pl.multiple_of(h * tall + i * step, 16), step)
                if m < 2:
                    ratio = jnp.concatenate([ratios[rows, :]] * (columns // 128), axis=1)
                else:
                    ratio = ratio_d
                new = params[m][rows, :] - learn_rate * (mn[m][rows, :] * ratio)
                mn[m][rows, :] = new
                hb[m][rows, :] = new.astype(bf16)

            src = hb[m].at[pl.ds(h * tall, tall)]
            at = piece(m, chip, k, h)
            for way, to in ((1, xn), (2, yn), (0, partner)):
                start(gather(m, h, way, src, at, to))
            copy = pltpu.make_async_copy(src, at, loc_sem.at[m, h])
            copy.start()
            local.append(copy)
        copy = pltpu.make_async_copy(mn[m], nexts[m], next_sem.at[m])
        copy.start()
        local.append(copy)

    def forward(m):
        at = await_piece(m, 0, 1, chip_x, k)
        start(gather(m, 0, 3, at, at, yn))
        start(gather(m, 0, 4, at, at, partner))
        at = await_piece(m, 1, 2, chip_y, k)
        start(gather(m, 1, 3, at, at, xn))
        start(gather(m, 1, 5, at, at, partner))

    def hand_over(m):
        at = await_piece(m, 1, 1, chip_x, k)
        start(gather(m, 1, 4, at, at, partner))
        at = await_piece(m, 0, 2, chip_y, k)
        start(gather(m, 0, 5, at, at, partner))
        for h in range(2):
            at = await_piece(m, h, 3, chip_d, k)
            start(gather(m, h, 6, at, at, partner))

    steps = len(jobs) // 2
    for t in range(steps + 2):
        for stage, lag in ((stage_1, 0), (stage_2, 1), (stage_3, 2)):
            if 0 <= t - lag < steps:
                for n in (2 * (t - lag), 2 * (t - lag) + 1):
                    stage(n)
        done, rest = divmod(t - 2 + 1, PIECES)
        if t >= 2 and rest == 0 and done >= 1:
            send_sizes(done - 1)
        done, rest = divmod(t - 2, PIECES)
        if t > 2 and rest == 0 and 1 <= done <= 2:
            update(done - 1)
    forward(0)
    update(2)

    for d in range(1, replicas):
        source = lax.rem(me + d, replicas)
        remote(nv_ref, nr.at[source], n_send.at[d - 1], n_recv.at[source], (source, z)).wait_recv()
    tall = hn_ref.shape[0]
    share = nn_ref.shape[0]
    total = nr[0, :tall]
    for n in range(1, replicas):
        total = total + nr[n, :tall]
    for n in range(replicas):
        rows = slice(n * share, (n + 1) * share)
        whole[rows, :] = nr[n, tall : tall + share] - learn_rate * (total[rows] * rate)
    hn_ref[...] = whole[...].astype(bf16)
    nn_ref[...] = whole[pl.ds(me * share, share), :]

    forward(1)
    forward(2)
    for m in range(3):
        hand_over(m)
    for m in range(3):
        for h in range(2):
            await_piece(m, h, 0, chip, 1 - k)
            await_piece(m, h, 4, chip_x, 1 - k)
            await_piece(m, h, 5, chip_y, 1 - k)
            await_piece(m, h, 6, chip_d, 1 - k)
    for copy in local:
        copy.wait()
    for copy in sent:
        copy.wait_send()


def fused(replicas, models):
    def run(
        slope_gate, slope_up, slope_down, slope_norm, param_gate, param_up, param_down, param_norm
    ):
        rows, columns = param_gate.shape
        tall, side = param_down.shape
        units = 2 * PIECES
        tall_n, share = slope_norm.shape[1] // 128, param_norm.shape[0] // 128
        pad = -(tall_n + share) % 8
        vectors = jnp.concatenate(
            [
                slope_norm.reshape(tall_n, 128),
                param_norm.reshape(share, 128),
                jnp.zeros((pad, 128), f32),
            ]
        )
        wide, deep = (rows // units, columns), (tall // units, side)
        V, DMA = pltpu.VMEM, pltpu.SemaphoreType.DMA
        by_chip = (2, replicas // 4, 2, rows, columns)
        shape = jax.ShapeDtypeStruct

        def three(front, dtype):
            return [V(front + wide, dtype), V(front + wide, dtype), V(front + deep, dtype)]

        out = pl.pallas_call(
            functools.partial(kernel, replicas, models),
            out_shape=(
                shape((rows * replicas, columns), bf16),
                shape((rows * replicas, columns), bf16),
                shape((tall, side * replicas), bf16),
                shape((rows, columns), f32),
                shape((rows, columns), f32),
                shape((tall, side), f32),
                shape((tall_n, 128), bf16),
                shape((share, 128), f32),
            ),
            in_specs=[pl.BlockSpec(memory_space=pl.ANY)] * 3
            + [pl.BlockSpec(memory_space=pltpu.VMEM)] * 4,
            out_specs=tuple(
                [pl.BlockSpec(memory_space=pl.ANY)] * 6
                + [pl.BlockSpec(memory_space=pltpu.VMEM)] * 2
            ),
            scratch_shapes=[
                *three((units, 2, 2), f32), *three((units, 2), bf16), *three((units, 2), bf16),
                *three((units,), bf16), *three((units,), bf16),
                V((rows, columns), f32), V((rows, columns), f32), V((tall, side), f32),
                V((SLOTS, 2, 2) + wide, f32), V((SLOTS, 2, 2) + deep, f32),
                V((rows, columns), bf16), V((rows, columns), bf16), V((tall, side), bf16),
                V((3, units, 2, 8, 128), f32), V((3, units, 2, 8, 128), f32),
                V((3, units, 8, 128), f32), V((3, units, 8, 128), f32),
                V((2, 2, rows, 128), f32), V((2, 8, side), f32),
                V((2, 2 * rows // 128, 128), f32), V((2, models - 1, 2 * rows // 128, 128), f32),
                V((models - 1, 2, 8, side), f32), V((rows, 128), f32),
                V((replicas,) + vectors.shape, f32), V((tall_n, 128), f32),
                DMA((3, units, 4)), DMA((3, units, 4)), DMA((3, units, 4)),
                DMA((3, units)), DMA((3, units)), DMA((3, units)), DMA((3, units)),
                DMA((3, units)), DMA((3, units)), DMA((3, units)), DMA((3, units)),
                DMA((3, models - 1)), DMA((3, models - 1)),
                DMA((replicas - 1,)), DMA((replicas,)),
                DMA((3, 2, 7)), DMA((3, 2, 7)), DMA((3, 2)), DMA((3,)),
            ],
            compiler_params=pltpu.CompilerParams(
                collective_id=0, has_side_effects=True, vmem_limit_bytes=67043328
            ),
        )(
            slope_gate.reshape(by_chip), slope_up.reshape(by_chip), slope_down[0],
            vectors, param_gate, param_up, param_down,
        )
        half_gate, half_up, half_down, next_gate, next_up, next_down, half_norm, next_norm = out
        return (
            half_gate, half_up, half_down, half_norm.reshape(-1),
            next_gate, next_up, next_down, next_norm.reshape(-1),
        )

    return run


def plain(
    slope_gate, slope_up, slope_down, slope_norm, param_gate, param_up, param_down, param_norm
):
    rate = lax.axis_size("replica") ** (-0.5)
    halves, nexts = [], []
    for slope, param, dim in (
        (slope_gate, param_gate, 0), (slope_up, param_up, 0), (slope_down, param_down, 1)
    ):
        mean = lax.psum_scatter(slope[0], "replica", scatter_dimension=dim, tiled=True) * rate
        own, size = lax.psum(
            (
                jnp.sum(param * param, axis=1 - dim, keepdims=True),
                jnp.sum(mean * mean, axis=1 - dim, keepdims=True),
            ),
            "model",
        )
        new = param - learn_rate * (mean * (jnp.sqrt(own) * lax.rsqrt(size + eps)))
        nexts.append(new)
        halves.append(lax.all_gather(new.astype(bf16), "replica", axis=dim, tiled=True))
    mean = lax.psum_scatter(slope_norm[0], "replica", scatter_dimension=0, tiled=True) * rate
    new = param_norm - learn_rate * mean
    nexts.append(new)
    halves.append(lax.all_gather(new.astype(bf16), "replica", axis=0, tiled=True))
    return (*halves, *nexts)


def solution(mesh):
    replicas, models = mesh.shape["replica"], mesh.shape["model"]
    body = fused(replicas, models) if replicas == 2 * 2 * 2 else plain
    matrix, turned = P("replica", "model"), P("model", "replica")
    return jax.shard_map(
        body,
        mesh=mesh,
        in_specs=(
            P("replica", None, "model"),
            P("replica", None, "model"),
            P("replica", "model", None),
            P("replica", None),
            matrix, matrix, turned, P("replica"),
        ),
        out_specs=(
            P(None, "model"), P(None, "model"), P("model", None), P(),
            matrix, matrix, turned, P("replica"),
        ),
        check_vma=False,
    )
```

```python
import functools

import jax
import jax.numpy as jnp
from jax import lax
from jax.experimental import pallas as pl
from jax.experimental.pallas import tpu as pltpu
from jax.sharding import PartitionSpec as P

learn_rate = 0.5
eps = 1e-06
MESH = pl.DeviceIdType.MESH
f32, bf16 = jnp.float32, jnp.bfloat16
PIECES = 2
SLOTS = 2
KERNEL_BYTES = 43000000
OCTAVES = 252.0
LOW = -125.0
LN2 = 0.6931471805599453


def tile_rows(columns, most=24576):
    return 16 * max(1, most // (16 * columns))


def tiles(shape):
    return [
        (slice(r, r + 16), slice(c, c + 128))
        for r in range(0, shape[0], 16)
        for c in range(0, shape[1], 128)
    ]


def largest(t):
    top = None
    for r in range(0, t.shape[0], 8):
        for c in range(0, t.shape[1], 128):
            part = jnp.abs(t[r : r + 8, c : c + 128])
            top = part if top is None else jnp.maximum(top, part)
    return top


def doubled(t):
    return jnp.concatenate([t, t], axis=0)


def encode(t, scale):
    power = jnp.exp2(jnp.abs(t) * scale + LOW)
    return jnp.where(t < 0, -power, power).astype(bf16)


def decode(t, slope, base):
    t = t.astype(f32)
    size = jnp.log(jnp.abs(t)) * slope + base
    return jnp.where(t < 0, -size, size)


def encoder(top):
    return doubled(OCTAVES / top)


def decoder(top):
    return doubled(top * (1.0 / (OCTAVES * LN2))), doubled(top * (-LOW / OCTAVES))


def decode_block(ref, start, shape, code):
    rows = []
    for r in range(0, shape[0], 16):
        at = pl.ds(pl.multiple_of(start + r, 16), 16)
        rows.append(
            jnp.concatenate(
                [decode(ref[at, c : c + 128], *code) for c in range(0, shape[1], 128)], axis=1
            )
        )
    return jnp.concatenate(rows, axis=0) if len(rows) > 1 else rows[0]


def settle(copies):
    for copy in copies:
        copy.wait_recv()


def kernel(
    replicas, models,
    g_ref, u_ref, d_ref, pg_ref, pu_ref, pd_ref, sn_ref, pn_ref,
    hg_ref, hu_ref, hd_ref, ng_ref, nu_ref, nd_ref, hn_ref, nn_ref,
    pr_g, pr_u, pr_d, r1_g, r1_u, r1_d, r2_g, r2_u, r2_d, pm_g, pm_u, pm_d,
    c1_w, c1_d, c2_w, c2_d, ow_w, ow_d, top1, got1, top2, got2,
    nrm_w, nrm_d, zs, zr_w, zr_d, ratios, nr, whole,
    ow_sem, pm_sem, pr_send, pr_recv, s1_send, s1_recv, s2_send, s2_recv,
    t1_send, t1_recv, t2_send, t2_recv,
    z_send, z_recv, n_send, n_recv, ag_send, ag_recv,
):
    me = lax.axis_index("replica")
    z = lax.axis_index("model")
    k = lax.rem(me, 2)
    x = lax.rem(me // 2, 2)
    y = me // 4
    partner = me + 1 - 2 * k
    xn = me + 2 - 4 * x
    yn = me + 4 - 8 * y
    rate = replicas ** (-0.5)

    slopes = (g_ref, u_ref, d_ref)
    halves = (hg_ref, hu_ref, hd_ref)
    mn = (ng_ref, nu_ref, nd_ref)
    pr, r1, r2 = (pr_g, pr_u, pr_d), (r1_g, r1_u, r1_d), (r2_g, r2_u, r2_d)
    params = (pm_g, pm_u, pm_d)
    units = 2 * PIECES
    side = nd_ref.shape[1]
    bands = ng_ref.shape[0] // 128

    others = [lax.rem(me + d, replicas) for d in range(1, replicas)]
    layers = [lax.rem(z + d, models) for d in range(1, models)]
    barrier = pltpu.get_barrier_semaphore()
    for other in others:
        pl.semaphore_signal(barrier, inc=1, device_id=(other, z), device_id_type=MESH)
    for layer in layers:
        pl.semaphore_signal(barrier, inc=1, device_id=(me, layer), device_id_type=MESH)

    sequence = [h * PIECES + j for j in range(PIECES) for h in range(2)]
    jobs = [(m, u) for m in range(3) for u in sequence]
    steps = len(jobs) // 2

    def remote(src, dst, send_sem, recv_sem, to):
        return pltpu.make_async_remote_copy(
            src_ref=src, dst_ref=dst, send_sem=send_sem, recv_sem=recv_sem,
            device_id=to, device_id_type=MESH,
        )

    sent = []

    def start(copy):
        copy.start()
        sent.append(copy)

    def height(m):
        return mn[m].shape[0] // units

    def parts(u):
        if u < PIECES:
            return [(1 - y, 1 - x), (y, 1 - x), (1 - y, x), (y, x)]
        return [(1 - y, 1 - x), (1 - y, x), (y, 1 - x), (y, x)]

    def view(m, u, q, core):
        rows = pl.ds(u * height(m), height(m))
        a, b = parts(u)[q]
        if m < 2:
            return slopes[m].at[a, b, core, rows, :]
        at = pl.multiple_of((2 * (2 * a + b) + core) * side, side)
        return slopes[m].at[rows, pl.ds(at, side)]

    def own_copy(n, q):
        m, u = jobs[n]
        ow = ow_w if m < 2 else ow_d
        return pltpu.make_async_copy(view(m, u, q, k), ow.at[n % SLOTS, q], ow_sem.at[m, u, q])

    def pair_copy(n, q):
        m, u = jobs[n]
        return remote(
            view(m, u, q, 1 - k), pr[m].at[u, q],
            pr_send.at[m, u, q], pr_recv.at[m, u, q], (partner, z),
        )

    for n in range(SLOTS):
        for q in range(4):
            own_copy(n, q).start()
    loads = [
        pltpu.make_async_copy(src, params[m], pm_sem.at[m])
        for m, src in enumerate((pg_ref, pu_ref, pd_ref))
    ]

    pl.semaphore_wait(barrier, replicas - 1 + models - 1)

    for q in range(2):
        for n in range(2):
            start(pair_copy(n, q))
    for n in range(2):
        for q in range(2, 4):
            start(pair_copy(n, q))
    for n in range(2, len(jobs)):
        for q in range(4):
            start(pair_copy(n, q))
    for copy in loads:
        copy.start()

    def slot_of(n):
        m = jobs[n][0]
        return (c1_w, c2_w, n % units) if m < 2 else (c1_d, c2_d, n % units)

    def first_copies(n, p):
        m, u = jobs[n]
        to = (xn if u < PIECES else yn, z)
        c1, _, slot = slot_of(n)
        return [
            remote(
                top1.at[m, u, p], got1.at[m, u, p], t1_send.at[m, u, p], t1_recv.at[m, u, p], to
            ),
            remote(
                c1.at[slot, p], r1[m].at[u, p], s1_send.at[m, u, p], s1_recv.at[m, u, p], to
            ),
        ]

    def second_copies(n):
        m, u = jobs[n]
        to = (yn if u < PIECES else xn, z)
        _, c2, slot = slot_of(n)
        return [
            remote(top2.at[m, u], got2.at[m, u], t2_send.at[m, u], t2_recv.at[m, u], to),
            remote(c2.at[slot], r2[m].at[u], s2_send.at[m, u], s2_recv.at[m, u], to),
        ]

    def reused(n):
        return jobs[n][0] == 1

    def sweep(m, body, carry=None):
        step = tile_rows(mn[m].shape[1])
        trips = height(m) // step
        if carry is None:
            pl.loop(0, trips)(lambda i: body(i * step, step))
            return None
        return lax.fori_loop(0, trips, lambda i, c: body(i * step, step, c), carry)

    def code_out(m, values, dst, top):
        scale = encoder(top)

        def body(at, step):
            for r in range(0, step, 16):
                rows = pl.ds(pl.multiple_of(at + r, 16), 16)
                for c in range(0, mn[m].shape[1], 128):
                    dst[rows, c : c + 128] = encode(values[rows, c : c + 128], scale)

        sweep(m, body)

    blank = jnp.full((8, 128), 1e-30, f32)

    def add(n, q, at, step):
        m, u = jobs[n]
        ow = ow_w if m < 2 else ow_d
        rows = pl.ds(pl.multiple_of(at, 16), step)
        both = pr[m][u, q, rows, :] + ow[n % SLOTS, q, rows, :]
        pr[m][u, q, rows, :] = both
        return both

    def stage_1(n, p):
        m, u = jobs[n]
        own_copy(n, p).wait()
        settle([pair_copy(n, p)])
        top = sweep(
            m, lambda at, step, c: jnp.maximum(c, largest(add(n, p, at, step))), blank
        )
        top1[m, u, p] = top
        c1, _, slot = slot_of(n)
        if reused(n):
            for copy in first_copies(n - units, p):
                copy.wait_send()
        code_out(m, pr[m].at[u, p], c1.at[slot, p], top)
        for copy in first_copies(n, p):
            copy.start()

    def stage_1_rest(n):
        m, u = jobs[n]
        for q in range(2, 4):
            own_copy(n, q).wait()
            settle([pair_copy(n, q)])

            def keep(at, step):
                add(n, q, at, step)

            sweep(m, keep)
        if n + SLOTS < len(jobs):
            for q in range(4):
                own_copy(n + SLOTS, q).start()

    def stage_2(n):
        m, u = jobs[n]
        settle(first_copies(n, 0))
        code = decoder(got1[m, u, 0])
        columns = mn[m].shape[1]

        def body(at, step, c):
            rows = pl.ds(pl.multiple_of(at, 16), step)
            both = pr[m][u, 2, rows, :] + decode_block(r1[m].at[u, 0], at, (step, columns), code)
            pr[m][u, 2, rows, :] = both
            return jnp.maximum(c, largest(both))

        top = sweep(m, body, blank)
        top2[m, u] = top
        _, c2, slot = slot_of(n)
        if reused(n):
            for copy in second_copies(n - units):
                copy.wait_send()
        code_out(m, pr[m].at[u, 2], c2.at[slot], top)
        for copy in second_copies(n):
            copy.start()

    def lanes(t):
        total = t[:, :128]
        for c in range(1, t.shape[1] // 128):
            total = total + t[:, c * 128 : (c + 1) * 128]
        return total

    def sublanes(t):
        total = t[:8]
        for c in range(1, t.shape[0] // 8):
            total = total + t[c * 8 : (c + 1) * 8]
        return total

    def stage_3(n):
        m, u = jobs[n]
        settle(first_copies(n, 1))
        settle(second_copies(n))
        columns = mn[m].shape[1]
        near, far = decoder(got1[m, u, 1]), decoder(got2[m, u])
        if u == sequence[0]:
            loads[m].wait()
            if m == 2:
                nrm_d[...] = jnp.zeros_like(nrm_d)

        def body(at, step):
            rows = pl.ds(pl.multiple_of(at, 16), step)
            here = pl.ds(pl.multiple_of(u * height(m) + at, 16), step)
            mean = pr[m][u, 3, rows, :] + decode_block(r1[m].at[u, 1], at, (step, columns), near)
            mean = (mean + decode_block(r2[m].at[u], at, (step, columns), far)) * rate
            param = params[m][here, :]
            mn[m][here, :] = mean
            if m < 2:
                nrm_w[0, here, :] = lanes(param * param)
                nrm_w[1, here, :] = lanes(mean * mean)
            else:
                nrm_d[0] = nrm_d[0] + sublanes(param * param)
                nrm_d[1] = nrm_d[1] + sublanes(mean * mean)

        sweep(m, body)

    def size_copies(m):
        src = zs.at[m] if m < 2 else nrm_d
        return [
            remote(
                src, zr_w.at[m, n] if m < 2 else zr_d.at[n],
                z_send.at[m, n], z_recv.at[m, n], (me, layer),
            )
            for n, layer in enumerate(layers)
        ]

    def send_sizes(m):
        if m < 2:
            for q in range(2):
                for b in range(bands):
                    block = nrm_w[q, b * 128 : (b + 1) * 128, :]
                    row = q * bands + b
                    zs[m, row : row + 1, :] = jnp.sum(block.T, axis=0, keepdims=True)
        for copy in size_copies(m):
            start(copy)

    def piece(m, chip, core, h):
        ref = halves[m]
        tall = mn[m].shape[0] // 2
        if m < 2:
            at = pl.multiple_of((2 * chip + core) * mn[0].shape[0], mn[0].shape[0])
            return ref.at[pl.ds(pl.multiple_of(at + h * tall, tall), tall), :]
        at = pl.multiple_of((2 * chip + core) * side, side)
        return ref.at[pl.ds(h * tall, tall), pl.ds(at, side)]

    chip, chip_x, chip_y, chip_d = me // 2, xn // 2, yn // 2, 3 - me // 2

    def gather(m, h, way, at, to):
        return remote(at, at, ag_send.at[m, h, way], ag_recv.at[m, h, way], (to, z))

    def await_piece(m, h, way, chip_from, core):
        at = piece(m, chip_from, core, h)
        settle([gather(m, h, way, at, partner)])
        return at

    def update(m):
        settle(size_copies(m))
        if m == 2:
            both = nrm_d[...]
            for n in range(models - 1):
                both = both + zr_d[n]
            own = jnp.sum(both[0], axis=0, keepdims=True)
            size = jnp.sum(both[1], axis=0, keepdims=True)
            ratio_d = jnp.sqrt(own) * lax.rsqrt(size + eps)
        else:
            both = zs[m]
            for n in range(models - 1):
                both = both + zr_w[m, n]
            ratio = jnp.sqrt(both[:bands]) * lax.rsqrt(both[bands : 2 * bands] + eps)
            for b in range(bands):
                ratios[b * 128 : (b + 1) * 128, :] = jnp.broadcast_to(
                    ratio[b : b + 1], (128, 128)
                ).T
        columns = mn[m].shape[1]
        step = tile_rows(columns)
        tall = mn[m].shape[0] // 2
        for h in range(2):
            at = piece(m, chip, k, h)

            @pl.loop(0, tall // step)
            def _(i):
                here = pl.ds(pl.multiple_of(i * step, 16), step)
                rows = pl.ds(pl.multiple_of(h * tall + i * step, 16), step)
                if m < 2:
                    ratio = jnp.concatenate([ratios[rows, :]] * (columns // 128), axis=1)
                else:
                    ratio = ratio_d
                new = params[m][rows, :] - learn_rate * (mn[m][rows, :] * ratio)
                mn[m][rows, :] = new
                at[here, :] = new.astype(bf16)

            for way, to in ((1, xn), (2, yn), (0, partner)):
                start(gather(m, h, way, at, to))

    def forward(m):
        at = await_piece(m, 0, 1, chip_x, k)
        start(gather(m, 0, 3, at, yn))
        start(gather(m, 0, 4, at, partner))
        at = await_piece(m, 1, 2, chip_y, k)
        start(gather(m, 1, 3, at, xn))
        start(gather(m, 1, 5, at, partner))

    def hand_over(m):
        at = await_piece(m, 1, 1, chip_x, k)
        start(gather(m, 1, 4, at, partner))
        at = await_piece(m, 0, 2, chip_y, k)
        start(gather(m, 0, 5, at, partner))
        for h in range(2):
            at = await_piece(m, h, 3, chip_d, k)
            start(gather(m, h, 6, at, partner))

    tall, share = hn_ref.shape[0], nn_ref.shape[0]

    def send_vectors():
        nr[me, :tall] = sn_ref[...]
        nr[me, tall:] = jnp.concatenate(
            [pn_ref[...], jnp.zeros((nr.shape[1] - tall - share, 128), f32)]
        )
        for n, other in enumerate(others):
            start(remote(nr.at[me], nr.at[me], n_send.at[n], n_recv.at[me], (other, z)))

    def finish_vectors():
        for d in range(1, replicas):
            source = lax.rem(me + d, replicas)
            at = nr.at[source]
            settle([remote(at, at, n_send.at[d - 1], n_recv.at[source], (source, z))])
        total = nr[0, :tall]
        for n in range(1, replicas):
            total = total + nr[n, :tall]
        for n in range(replicas):
            rows = slice(n * share, (n + 1) * share)
            whole[rows, :] = nr[n, tall : tall + share] - learn_rate * (total[rows] * rate)
        hn_ref[...] = whole[...].astype(bf16)
        nn_ref[...] = whole[pl.ds(me * share, share), :]

    for t in range(steps + 2):
        if t < steps:
            for p in range(2):
                for n in (2 * t, 2 * t + 1):
                    stage_1(n, p)
            for n in (2 * t, 2 * t + 1):
                stage_1_rest(n)
        if t == 0:
            send_vectors()
        for stage, lag in ((stage_2, 1), (stage_3, 2)):
            if 0 <= t - lag < steps:
                for n in (2 * (t - lag), 2 * (t - lag) + 1):
                    stage(n)
        done, rest = divmod(t - 2 + 1, PIECES)
        if t >= 2 and rest == 0 and done >= 1:
            send_sizes(done - 1)
        done, rest = divmod(t - 2, PIECES)
        if t > 2 and rest == 0 and 1 <= done <= 2:
            update(done - 1)
    forward(0)
    update(2)
    finish_vectors()
    forward(1)
    forward(2)
    for m in range(3):
        hand_over(m)
    for m in range(3):
        for h in range(2):
            await_piece(m, h, 0, chip, 1 - k)
            await_piece(m, h, 4, chip_x, 1 - k)
            await_piece(m, h, 5, chip_y, 1 - k)
            await_piece(m, h, 6, chip_d, 1 - k)
    for n in range(len(jobs)):
        if n + units >= len(jobs) or not reused(n + units):
            for copy in first_copies(n, 0) + first_copies(n, 1) + second_copies(n):
                copy.wait_send()
    for copy in sent:
        copy.wait_send()


def put(*refs):
    count = len(refs) // 2
    ins, outs, sem = refs[:count], refs[count : 2 * count], refs[2 * count]
    copies = [
        pltpu.make_async_copy(src, dst, sem.at[n])
        for n, (src, dst) in enumerate(zip(ins, outs))
    ]
    for copy in copies:
        copy.start()
    for copy in copies:
        copy.wait()


def fused(replicas, models):
    def run(
        slope_gate, slope_up, slope_down, slope_norm, param_gate, param_up, param_down, param_norm
    ):
        rows, columns = param_gate.shape
        tall, side = param_down.shape
        units = 2 * PIECES
        tall_n, share = slope_norm.shape[1] // 128, param_norm.shape[0] // 128
        lines = tall_n + share + -(tall_n + share) % 8
        wide, deep = (rows // units, columns), (tall // units, side)
        V, DMA = pltpu.VMEM, pltpu.SemaphoreType.DMA
        by_chip = (2, replicas // 4, 2, rows, columns)
        whole, inside = pl.BlockSpec(memory_space=pl.ANY), pl.BlockSpec(memory_space=pltpu.VMEM)

        def three(front, dtype):
            return [V(front + wide, dtype), V(front + wide, dtype), V(front + deep, dtype)]

        out = pl.pallas_call(
            functools.partial(kernel, replicas, models),
            out_shape=(
                V((rows * replicas, columns), bf16),
                V((rows * replicas, columns), bf16),
                V((tall, side * replicas), bf16),
                V((rows, columns), f32),
                V((rows, columns), f32),
                V((tall, side), f32),
                V((tall_n, 128), bf16),
                V((share, 128), f32),
            ),
            in_specs=[whole] * 6 + [inside] * 2,
            out_specs=tuple([inside] * 8),
            scratch_shapes=[
                *three((units, 4), f32), *three((units, 2), bf16), *three((units,), bf16),
                V((rows, columns), f32), V((rows, columns), f32), V((tall, side), f32),
                V((units, 2) + wide, bf16), V((units, 2) + deep, bf16),
                V((units,) + wide, bf16), V((units,) + deep, bf16),
                V((SLOTS, 4) + wide, f32), V((SLOTS, 4) + deep, f32),
                V((3, units, 2, 8, 128), f32), V((3, units, 2, 8, 128), f32),
                V((3, units, 8, 128), f32), V((3, units, 8, 128), f32),
                V((2, rows, 128), f32), V((2, 8, side), f32),
                V((2, 2 * rows // 128, 128), f32), V((2, models - 1, 2 * rows // 128, 128), f32),
                V((models - 1, 2, 8, side), f32), V((rows, 128), f32),
                V((replicas, lines, 128), f32), V((tall_n, 128), f32),
                DMA((3, units, 4)), DMA((3,)), DMA((3, units, 4)), DMA((3, units, 4)),
                DMA((3, units, 2)), DMA((3, units, 2)), DMA((3, units)), DMA((3, units)),
                DMA((3, units, 2)), DMA((3, units, 2)), DMA((3, units)), DMA((3, units)),
                DMA((3, models - 1)), DMA((3, models - 1)),
                DMA((replicas - 1,)), DMA((replicas,)),
                DMA((3, 2, 7)), DMA((3, 2, 7)),
            ],
            compiler_params=pltpu.CompilerParams(
                collective_id=0, has_side_effects=True, vmem_limit_bytes=KERNEL_BYTES
            ),
        )(
            slope_gate.reshape(by_chip), slope_up.reshape(by_chip), slope_down[0],
            param_gate, param_up, param_down,
            slope_norm.reshape(tall_n, 128), param_norm.reshape(share, 128),
        )
        half_gate, half_up, half_down, next_gate, next_up, next_down, half_norm, next_norm = (
            pl.pallas_call(
                put,
                out_shape=tuple(jax.ShapeDtypeStruct(o.shape, o.dtype) for o in out),
                in_specs=[inside] * len(out),
                out_specs=tuple([whole] * len(out)),
                scratch_shapes=[DMA((len(out),))],
                compiler_params=pltpu.CompilerParams(vmem_limit_bytes=1 << 20),
            )(*[pltpu.with_memory_space_constraint(o, pltpu.VMEM) for o in out])
        )
        return (
            half_gate, half_up, half_down, half_norm.reshape(-1),
            next_gate, next_up, next_down, next_norm.reshape(-1),
        )

    return run


def plain(
    slope_gate, slope_up, slope_down, slope_norm, param_gate, param_up, param_down, param_norm
):
    rate = lax.axis_size("replica") ** (-0.5)
    halves, nexts = [], []
    for slope, param, dim in (
        (slope_gate, param_gate, 0), (slope_up, param_up, 0), (slope_down, param_down, 1)
    ):
        mean = lax.psum_scatter(slope[0], "replica", scatter_dimension=dim, tiled=True) * rate
        own, size = lax.psum(
            (
                jnp.sum(param * param, axis=1 - dim, keepdims=True),
                jnp.sum(mean * mean, axis=1 - dim, keepdims=True),
            ),
            "model",
        )
        new = param - learn_rate * (mean * (jnp.sqrt(own) * lax.rsqrt(size + eps)))
        nexts.append(new)
        halves.append(lax.all_gather(new.astype(bf16), "replica", axis=dim, tiled=True))
    mean = lax.psum_scatter(slope_norm[0], "replica", scatter_dimension=0, tiled=True) * rate
    new = param_norm - learn_rate * mean
    nexts.append(new)
    halves.append(lax.all_gather(new.astype(bf16), "replica", axis=0, tiled=True))
    return (*halves, *nexts)


def solution(mesh):
    replicas, models = mesh.shape["replica"], mesh.shape["model"]
    body = fused(replicas, models) if replicas == 2 * 2 * 2 else plain
    matrix, turned = P("replica", "model"), P("model", "replica")
    return jax.shard_map(
        body,
        mesh=mesh,
        in_specs=(
            P("replica", None, "model"),
            P("replica", None, "model"),
            P("replica", "model", None),
            P("replica", None),
            matrix, matrix, turned, P("replica"),
        ),
        out_specs=(
            P(None, "model"), P(None, "model"), P("model", None), P(),
            matrix, matrix, turned, P("replica"),
        ),
        check_vma=False,
    )
```

```python
import functools

import jax
import jax.numpy as jnp
from jax import lax
from jax.experimental import pallas as pl
from jax.experimental.pallas import tpu as pltpu
from jax.sharding import PartitionSpec as P

learn_rate = 0.5
eps = 1e-06
MESH = pl.DeviceIdType.MESH
f32, bf16 = jnp.float32, jnp.bfloat16
PIECES = 2
SLOTS = 2
KERNEL_BYTES = 43000000
BEND = 15.0
POWER = 63.0
FLOOR = 125 * 0.6931471805599453
TINY = 1e-30


def tile_rows(columns, most=24576):
    return 16 * max(1, most // (16 * columns))


def doubled(t):
    return jnp.concatenate([t, t], axis=0)


def limit(top):
    return (top * (1 + 2**-7)).astype(bf16)


def encode(t, scale):
    size = jnp.exp(POWER * jnp.log(1 + jnp.abs(t) * scale) - FLOOR)
    return jnp.where(t < 0, -size, size).astype(bf16)


def decode(t, scale):
    t = t.astype(f32)
    size = (jnp.exp((jnp.log(jnp.abs(t)) + FLOOR) * (1 / POWER)) - 1) * scale
    return jnp.where(t < 0, -size, size)


def coded_at(row, column, wide):
    return pl.ds(pl.multiple_of(row * wide + column * 16, 16), 16)


def settle(copies):
    for copy in copies:
        copy.wait_recv()


def kernel(
    replicas, models,
    g_ref, u_ref, d_ref, pg_ref, pu_ref, pd_ref, sn_ref, pn_ref,
    hg_ref, hu_ref, hd_ref, ng_ref, nu_ref, nd_ref, hn_ref, nn_ref,
    pr_g, pr_u, pr_d, pm_g, pm_u, pm_d, c1, r1, c2, r2, ow_w, ow_d,
    nrm_w, nrm_d, zs, zr_w, zr_d, ratios, nr, whole,
    ow_sem, pm_sem, pr_send, pr_recv, s1_send, s1_recv, s2_send, s2_recv,
    z_send, z_recv, n_send, n_recv, ag_send, ag_recv, ag_pair,
):
    me = lax.axis_index("replica")
    z = lax.axis_index("model")
    k = lax.rem(me, 2)
    x = lax.rem(me // 2, 2)
    y = me // 4
    partner = me + 1 - 2 * k
    xn = me + 2 - 4 * x
    yn = me + 4 - 8 * y
    rate = replicas ** (-0.5)

    slopes = (g_ref, u_ref, d_ref)
    halves = (hg_ref, hu_ref, hd_ref)
    mn = (ng_ref, nu_ref, nd_ref)
    pr = (pr_g, pr_u, pr_d)
    params = (pm_g, pm_u, pm_d)
    units = 2 * PIECES
    side = nd_ref.shape[1]
    bands = ng_ref.shape[0] // 128

    others = [lax.rem(me + d, replicas) for d in range(1, replicas)]
    layers = [lax.rem(z + d, models) for d in range(1, models)]
    barrier = pltpu.get_barrier_semaphore()
    for other in others:
        pl.semaphore_signal(barrier, inc=1, device_id=(other, z), device_id_type=MESH)
    for layer in layers:
        pl.semaphore_signal(barrier, inc=1, device_id=(me, layer), device_id_type=MESH)

    sequence = [h * PIECES + j for j in range(PIECES) for h in range(2)]
    jobs = [(m, u) for m in range(3) for u in sequence]
    steps = len(jobs) // 2

    def remote(src, dst, send_sem, recv_sem, to):
        return pltpu.make_async_remote_copy(
            src_ref=src, dst_ref=dst, send_sem=send_sem, recv_sem=recv_sem,
            device_id=to, device_id_type=MESH,
        )

    def height(m):
        return mn[m].shape[0] // units

    def parts(u):
        if u < PIECES:
            return [(1 - y, 1 - x), (y, 1 - x), (1 - y, x), (y, x)]
        return [(1 - y, 1 - x), (1 - y, x), (y, 1 - x), (y, x)]

    def view(m, u, q, core):
        rows = pl.ds(u * height(m), height(m))
        a, b = parts(u)[q]
        if m < 2:
            return slopes[m].at[a, b, core, rows, :]
        at = pl.multiple_of((2 * (2 * a + b) + core) * side, side)
        return slopes[m].at[rows, pl.ds(at, side)]

    def own_copy(n, q):
        m, u = jobs[n]
        ow = ow_w if m < 2 else ow_d
        return pltpu.make_async_copy(view(m, u, q, k), ow.at[n % SLOTS, q], ow_sem.at[n % SLOTS, q])

    def pair_copy(n, q):
        m, u = jobs[n]
        sem = 3 * n + min(q, 2) if n < units else 2 * units + n
        return remote(
            view(m, u, q, 1 - k), pr[m].at[u, q], pr_send.at[m], pr_recv.at[sem], (partner, z)
        )

    def await_pair(n, q):
        m, u = jobs[n]
        if n < units:
            at = pr[m].at[u, q] if q < 2 else pr[m].at[u, pl.ds(2, 2)]
            settle([remote(at, at, pr_send.at[m], pr_recv.at[3 * n + q], (partner, z))])
        elif q == 0:
            at = pr[m].at[u]
            settle([remote(at, at, pr_send.at[m], pr_recv.at[2 * units + n], (partner, z))])

    for n in range(SLOTS):
        for q in range(4):
            own_copy(n, q).start()
    loads = [
        pltpu.make_async_copy(src, params[m], pm_sem.at[m])
        for m, src in enumerate((pg_ref, pu_ref, pd_ref))
    ]

    pl.semaphore_wait(barrier, replicas - 1 + models - 1)

    for q in range(2):
        for n in range(2):
            pair_copy(n, q).start()
    for n in range(2):
        for q in range(2, 4):
            pair_copy(n, q).start()
    for n in range(2, len(jobs)):
        for q in range(4):
            pair_copy(n, q).start()
    for copy in loads:
        copy.start()

    def first_copy(n, p):
        m, u = jobs[n]
        return remote(
            c1.at[n % units, p], r1.at[m, u, p], s1_send.at[n % units, p],
            s1_recv.at[n] if p == 0 else s2_recv.at[n], (xn if u < PIECES else yn, z),
        )

    def second_copy(n):
        m, u = jobs[n]
        return remote(
            c2.at[n % units], r2.at[m, u], s2_send.at[n % units], s2_recv.at[n],
            (yn if u < PIECES else xn, z),
        )

    def await_rest(n):
        at = r1.at[jobs[n]]
        settle([remote(at, at, s2_send.at[n % units], s2_recv.at[n], (xn, z))])

    def sweep(m, body, carry=None):
        step = tile_rows(mn[m].shape[1])
        trips = height(m) // step
        if carry is None:
            pl.loop(0, trips)(lambda i: body(i * step, step))
            return None
        return lax.fori_loop(0, trips, lambda i, c: body(i * step, step, c), carry)

    def code_rows(m, read, dst):
        wide = mn[m].shape[1] // 128
        lane = lax.broadcasted_iota(jnp.int32, (16, 128), 1)

        def body(at, step, tops):
            values = read(at, step)
            for r in range(0, step, 16):
                line = [values[r : r + 16, c * 128 : (c + 1) * 128] for c in range(wide)]
                top = functools.reduce(jnp.maximum, [jnp.abs(t) for t in line])
                top = jnp.maximum(jnp.max(top, axis=1, keepdims=True), TINY)
                top = limit(jnp.broadcast_to(top, (16, 128))).astype(f32)
                scale = BEND / top
                for c, t in enumerate(line):
                    dst[coded_at(at + r, c, wide), :] = encode(t, scale)
                tops = jnp.where(lane == (at + r) // 16, top, tops)
            return tops

        tops = sweep(m, body, jnp.full((16, 128), TINY, f32))
        dst[dst.shape[0] - 16 :, :] = tops.astype(bf16)

    def code_columns(m, read, values, dst):
        wide = mn[m].shape[1] // 128

        def highest(at, step, tops):
            t = jnp.abs(read(at, step))
            for r in range(0, step, 8):
                tops = jnp.maximum(tops, t[r : r + 8])
            return tops

        tops = sweep(m, highest, jnp.full((8, wide * 128), TINY, f32))
        tops = limit(jnp.broadcast_to(jnp.max(tops, axis=0, keepdims=True), tops.shape))
        tops = tops.astype(f32)
        each = [tops[:, c * 128 : (c + 1) * 128] for c in range(wide)]
        scales = [doubled(BEND / top) for top in each]
        dst[dst.shape[0] - 16 :, :] = jnp.concatenate(each, axis=0).astype(bf16)

        def body(at, step):
            for r in range(0, step, 16):
                rows = pl.ds(pl.multiple_of(at + r, 16), 16)
                for c in range(wide):
                    t = values[rows, c * 128 : (c + 1) * 128]
                    dst[coded_at(at + r, c, wide), :] = encode(t, scales[c])

        sweep(m, body)

    def code_out(m, read, values, dst):
        if m < 2:
            code_rows(m, read, dst)
        else:
            code_columns(m, read, values, dst)

    def scales_of(m, src, at):
        tops = src[src.shape[0] - 16 :, :].astype(f32) * (1 / BEND)
        wide = mn[m].shape[1] // 128
        if m == 2:
            each = [doubled(tops[c * 8 : (c + 1) * 8]) for c in range(wide)]
            return lambda r: each
        lane = lax.broadcasted_iota(jnp.int32, (16, 128), 1)

        def of(r):
            top = jnp.where(lane == (at + r) // 16, tops, 0)
            return [jnp.broadcast_to(jnp.max(top, axis=1, keepdims=True), (16, 128))] * wide

        return of

    def decoded(m, src, at, step):
        wide = mn[m].shape[1] // 128
        of = scales_of(m, src, at)
        rows = []
        for r in range(0, step, 16):
            scales = of(r)
            line = [decode(src[coded_at(at + r, c, wide), :], scales[c]) for c in range(wide)]
            rows.append(jnp.concatenate(line, axis=1))
        return jnp.concatenate(rows, axis=0) if len(rows) > 1 else rows[0]

    def add(n, q, at, step):
        m, u = jobs[n]
        ow = ow_w if m < 2 else ow_d
        rows = pl.ds(pl.multiple_of(at, 16), step)
        both = pr[m][u, q, rows, :] + ow[n % SLOTS, q, rows, :]
        if m == 2 or q >= 2:
            pr[m][u, q, rows, :] = both
        return both

    def stage_1(n, p):
        m, u = jobs[n]
        own_copy(n, p).wait()
        await_pair(n, p)
        if n >= units:
            first_copy(n - units, p).wait_send()
        code_out(
            m, lambda at, step: add(n, p, at, step), pr[m].at[u, p], c1.at[n % units, p]
        )
        first_copy(n, p).start()

    def stage_1_rest(n):
        m, u = jobs[n]
        await_pair(n, 2)
        for q in range(2, 4):
            own_copy(n, q).wait()

            def keep(at, step):
                add(n, q, at, step)

            sweep(m, keep)
        if n + SLOTS < len(jobs):
            for q in range(4):
                own_copy(n + SLOTS, q).start()

    def stage_2(n):
        m, u = jobs[n]
        settle([first_copy(n, 0)])

        def both(at, step):
            rows = pl.ds(pl.multiple_of(at, 16), step)
            total = pr[m][u, 2, rows, :] + decoded(m, r1.at[m, u, 0], at, step)
            if m == 2:
                pr[m][u, 2, rows, :] = total
            return total

        if n >= units:
            second_copy(n - units).wait_send()
        code_out(m, both, pr[m].at[u, 2], c2.at[n % units])
        second_copy(n).start()

    def lanes(t):
        total = t[:, :128]
        for c in range(1, t.shape[1] // 128):
            total = total + t[:, c * 128 : (c + 1) * 128]
        return total

    def sublanes(t):
        total = t[:8]
        for c in range(1, t.shape[0] // 8):
            total = total + t[c * 8 : (c + 1) * 8]
        return total

    def stage_3(n):
        m, u = jobs[n]
        await_rest(n)
        if u == sequence[0]:
            loads[m].wait()
            if m == 2:
                nrm_d[...] = jnp.zeros_like(nrm_d)

        def body(at, step):
            rows = pl.ds(pl.multiple_of(at, 16), step)
            here = pl.ds(pl.multiple_of(u * height(m) + at, 16), step)
            mean = pr[m][u, 3, rows, :] + decoded(m, r1.at[m, u, 1], at, step)
            mean = (mean + decoded(m, r2.at[m, u], at, step)) * rate
            param = params[m][here, :]
            mn[m][here, :] = mean
            if m < 2:
                nrm_w[0, here, :] = lanes(param * param)
                nrm_w[1, here, :] = lanes(mean * mean)
            else:
                nrm_d[0] = nrm_d[0] + sublanes(param * param)
                nrm_d[1] = nrm_d[1] + sublanes(mean * mean)

        sweep(m, body)

    def size_copies(m):
        src = zs.at[m] if m < 2 else nrm_d
        return [
            remote(
                src, zr_w.at[m, n] if m < 2 else zr_d.at[n],
                z_send.at[m], z_recv.at[m], (me, layer),
            )
            for n, layer in enumerate(layers)
        ]

    def all_sizes(m):
        at = zr_w.at[m] if m < 2 else zr_d
        return remote(at, at, z_send.at[m], z_recv.at[m], (me, layers[0]))

    def send_sizes(m):
        if m < 2:
            for q in range(2):
                for b in range(bands):
                    block = nrm_w[q, b * 128 : (b + 1) * 128, :]
                    row = q * bands + b
                    zs[m, row : row + 1, :] = jnp.sum(block.T, axis=0, keepdims=True)
        for copy in size_copies(m):
            copy.start()

    def piece(m, chip, core, h):
        ref = halves[m]
        tall = mn[m].shape[0] // 2
        if m < 2:
            at = pl.multiple_of((2 * chip + core) * mn[0].shape[0], mn[0].shape[0])
            return ref.at[pl.ds(pl.multiple_of(at + h * tall, tall), tall), :]
        at = pl.multiple_of((2 * chip + core) * side, side)
        return ref.at[pl.ds(h * tall, tall), pl.ds(at, side)]

    chip, chip_x, chip_y, chip_d = me // 2, xn // 2, yn // 2, 3 - me // 2

    def gather(m, h, way, at, to):
        sem = ag_recv.at[m, h, way] if way < 3 else ag_pair.at[m]
        return remote(at, at, ag_send.at[m], sem, (to, z))

    def gathered(m, count):
        rows, columns = mn[m].shape
        if m < 2:
            at = halves[m].at[pl.ds(0, rows * count // 2), :]
        else:
            at = halves[m].at[:, pl.ds(0, columns * count // 2)]
        return remote(at, at, ag_send.at[m], ag_pair.at[m], (partner, z))

    def await_piece(m, h, way, chip_from, core):
        at = piece(m, chip_from, core, h)
        settle([gather(m, h, way, at, partner)])
        return at

    def update(m):
        settle([all_sizes(m)])
        if m == 2:
            both = nrm_d[...]
            for n in range(models - 1):
                both = both + zr_d[n]
            own = jnp.sum(both[0], axis=0, keepdims=True)
            size = jnp.sum(both[1], axis=0, keepdims=True)
            ratio_d = jnp.sqrt(own) * lax.rsqrt(size + eps)
        else:
            both = zs[m]
            for n in range(models - 1):
                both = both + zr_w[m, n]
            ratio = jnp.sqrt(both[:bands]) * lax.rsqrt(both[bands : 2 * bands] + eps)
            for b in range(bands):
                ratios[b * 128 : (b + 1) * 128, :] = jnp.broadcast_to(
                    ratio[b : b + 1], (128, 128)
                ).T
        columns = mn[m].shape[1]
        step = tile_rows(columns)
        tall = mn[m].shape[0] // 2
        for h in range(2):
            at = piece(m, chip, k, h)

            @pl.loop(0, tall // step)
            def _(i):
                here = pl.ds(pl.multiple_of(i * step, 16), step)
                rows = pl.ds(pl.multiple_of(h * tall + i * step, 16), step)
                if m < 2:
                    ratio = jnp.concatenate([ratios[rows, :]] * (columns // 128), axis=1)
                else:
                    ratio = ratio_d
                new = params[m][rows, :] - learn_rate * (mn[m][rows, :] * ratio)
                mn[m][rows, :] = new
                at[here, :] = new.astype(bf16)

            for way, to in ((0, xn), (1, yn), (3, partner)):
                gather(m, h, way, at, to).start()

    def relay(m, h, way, chip_from, *targets):
        at = await_piece(m, h, way, chip_from, k)
        for to_way, to in targets:
            gather(m, h, to_way, at, to).start()

    def forward(m):
        relay(m, 0, 0, chip_x, (2, yn), (3, partner))
        relay(m, 1, 1, chip_y, (2, xn), (3, partner))

    def hand_over(m):
        relay(m, 1, 0, chip_x, (3, partner))
        relay(m, 0, 1, chip_y, (3, partner))
        for h in range(2):
            relay(m, h, 2, chip_d, (3, partner))

    tall, share = hn_ref.shape[0], nn_ref.shape[0]

    def all_vectors():
        at = nr.at[pl.ds(0, replicas - 1)]
        return remote(at, at, n_send.at[0], n_recv.at[0], (partner, z))

    def send_vectors():
        nr[me, :tall] = sn_ref[...]
        nr[me, tall:] = jnp.concatenate(
            [pn_ref[...], jnp.zeros((nr.shape[1] - tall - share, 128), f32)]
        )
        for other in others:
            remote(nr.at[me], nr.at[me], n_send.at[0], n_recv.at[0], (other, z)).start()

    def finish_vectors():
        settle([all_vectors()])
        total = nr[0, :tall]
        for n in range(1, replicas):
            total = total + nr[n, :tall]
        for n in range(replicas):
            rows = slice(n * share, (n + 1) * share)
            whole[rows, :] = nr[n, tall : tall + share] - learn_rate * (total[rows] * rate)
        hn_ref[...] = whole[...].astype(bf16)
        nn_ref[...] = whole[pl.ds(me * share, share), :]

    for t in range(steps + 2):
        if t < steps:
            for p in range(2):
                for n in (2 * t, 2 * t + 1):
                    stage_1(n, p)
            for n in (2 * t, 2 * t + 1):
                stage_1_rest(n)
        if t == 0:
            send_vectors()
        for stage, lag in ((stage_2, 1), (stage_3, 2)):
            if 0 <= t - lag < steps:
                for n in (2 * (t - lag), 2 * (t - lag) + 1):
                    stage(n)
        done, rest = divmod(t - 2 + 1, PIECES)
        if t >= 2 and rest == 0 and done >= 1:
            send_sizes(done - 1)
        done, rest = divmod(t - 2, PIECES)
        if t > 2 and rest == 0 and 1 <= done <= 2:
            update(done - 1)
    forward(0)
    update(2)
    finish_vectors()
    forward(1)
    forward(2)
    for m in range(3):
        hand_over(m)
    for m in range(3):
        settle([gathered(m, replicas)])
    for n in range(len(jobs) - units, len(jobs)):
        for p in range(2):
            first_copy(n, p).wait_send()
        second_copy(n).wait_send()
    for m in range(3):
        remote(pr[m], pr[m], pr_send.at[m], pr_recv.at[0], (partner, z)).wait_send()
        all_sizes(m).wait_send()
        gathered(m, 2 * replicas - 2).wait_send()
    all_vectors().wait_send()


def put(*refs):
    count = len(refs) // 2
    ins, outs, sem = refs[:count], refs[count : 2 * count], refs[2 * count]
    copies = [
        pltpu.make_async_copy(src, dst, sem.at[n])
        for n, (src, dst) in enumerate(zip(ins, outs))
    ]
    for copy in copies:
        copy.start()
    for copy in copies:
        copy.wait()


def fused(replicas, models):
    def run(
        slope_gate, slope_up, slope_down, slope_norm, param_gate, param_up, param_down, param_norm
    ):
        rows, columns = param_gate.shape
        tall, side = param_down.shape
        units = 2 * PIECES
        tall_n, share = slope_norm.shape[1] // 128, param_norm.shape[0] // 128
        lines = tall_n + share + -(tall_n + share) % 8
        wide, deep = (rows // units, columns), (tall // units, side)
        coded = (rows // units * columns // 128 + 16, 128)
        V, DMA = pltpu.VMEM, pltpu.SemaphoreType.DMA
        by_chip = (2, replicas // 4, 2, rows, columns)
        whole, inside = pl.BlockSpec(memory_space=pl.ANY), pl.BlockSpec(memory_space=pltpu.VMEM)

        def three(front, dtype):
            return [V(front + wide, dtype), V(front + wide, dtype), V(front + deep, dtype)]

        out = pl.pallas_call(
            functools.partial(kernel, replicas, models),
            out_shape=(
                V((rows * replicas, columns), bf16),
                V((rows * replicas, columns), bf16),
                V((tall, side * replicas), bf16),
                V((rows, columns), f32),
                V((rows, columns), f32),
                V((tall, side), f32),
                V((tall_n, 128), bf16),
                V((share, 128), f32),
            ),
            in_specs=[whole] * 6 + [inside] * 2,
            out_specs=tuple([inside] * 8),
            scratch_shapes=[
                *three((units, 4), f32),
                V((rows, columns), f32), V((rows, columns), f32), V((tall, side), f32),
                V((units, 2) + coded, bf16), V((3, units, 2) + coded, bf16),
                V((units,) + coded, bf16), V((3, units) + coded, bf16),
                V((SLOTS, 4) + wide, f32), V((SLOTS, 4) + deep, f32),
                V((2, rows, 128), f32), V((2, 8, side), f32),
                V((2, 2 * rows // 128, 128), f32), V((2, models - 1, 2 * rows // 128, 128), f32),
                V((models - 1, 2, 8, side), f32), V((rows, 128), f32),
                V((replicas, lines, 128), f32), V((tall_n, 128), f32),
                DMA((SLOTS, 4)), DMA((3,)), DMA((3,)), DMA((5 * units,)),
                DMA((units, 2)), DMA((3 * units,)), DMA((units,)), DMA((3 * units,)),
                DMA((3,)), DMA((3,)), DMA((1,)), DMA((1,)),
                DMA((3,)), DMA((3, 2, 3)), DMA((3,)),
            ],
            compiler_params=pltpu.CompilerParams(
                collective_id=0, has_side_effects=True, vmem_limit_bytes=KERNEL_BYTES
            ),
        )(
            slope_gate.reshape(by_chip), slope_up.reshape(by_chip), slope_down[0],
            param_gate, param_up, param_down,
            slope_norm.reshape(tall_n, 128), param_norm.reshape(share, 128),
        )
        half_gate, half_up, half_down, next_gate, next_up, next_down, half_norm, next_norm = (
            pl.pallas_call(
                put,
                out_shape=tuple(jax.ShapeDtypeStruct(o.shape, o.dtype) for o in out),
                in_specs=[inside] * len(out),
                out_specs=tuple([whole] * len(out)),
                scratch_shapes=[DMA((len(out),))],
                compiler_params=pltpu.CompilerParams(vmem_limit_bytes=1 << 20),
            )(*[pltpu.with_memory_space_constraint(o, pltpu.VMEM) for o in out])
        )
        return (
            half_gate, half_up, half_down, half_norm.reshape(-1),
            next_gate, next_up, next_down, next_norm.reshape(-1),
        )

    return run


def plain(
    slope_gate, slope_up, slope_down, slope_norm, param_gate, param_up, param_down, param_norm
):
    rate = lax.axis_size("replica") ** (-0.5)
    halves, nexts = [], []
    for slope, param, dim in (
        (slope_gate, param_gate, 0), (slope_up, param_up, 0), (slope_down, param_down, 1)
    ):
        mean = lax.psum_scatter(slope[0], "replica", scatter_dimension=dim, tiled=True) * rate
        own, size = lax.psum(
            (
                jnp.sum(param * param, axis=1 - dim, keepdims=True),
                jnp.sum(mean * mean, axis=1 - dim, keepdims=True),
            ),
            "model",
        )
        new = param - learn_rate * (mean * (jnp.sqrt(own) * lax.rsqrt(size + eps)))
        nexts.append(new)
        halves.append(lax.all_gather(new.astype(bf16), "replica", axis=dim, tiled=True))
    mean = lax.psum_scatter(slope_norm[0], "replica", scatter_dimension=0, tiled=True) * rate
    new = param_norm - learn_rate * mean
    nexts.append(new)
    halves.append(lax.all_gather(new.astype(bf16), "replica", axis=0, tiled=True))
    return (*halves, *nexts)


def solution(mesh):
    replicas, models = mesh.shape["replica"], mesh.shape["model"]
    body = fused(replicas, models) if replicas == 2 * 2 * 2 else plain
    matrix, turned = P("replica", "model"), P("model", "replica")
    return jax.shard_map(
        body,
        mesh=mesh,
        in_specs=(
            P("replica", None, "model"),
            P("replica", None, "model"),
            P("replica", "model", None),
            P("replica", None),
            matrix, matrix, turned, P("replica"),
        ),
        out_specs=(
            P(None, "model"), P(None, "model"), P("model", None), P(),
            matrix, matrix, turned, P("replica"),
        ),
        check_vma=False,
    )
```

```python
import functools

import jax
import jax.numpy as jnp
from jax import lax
from jax.experimental import pallas as pl
from jax.experimental.pallas import tpu as pltpu
from jax.sharding import PartitionSpec as P

learn_rate = 0.5
eps = 1e-06
MESH = pl.DeviceIdType.MESH
f32, bf16 = jnp.float32, jnp.bfloat16
PIECES = 2
SLOTS = 2
KERNEL_BYTES = 43000000
BEND = 15.0
POWER = 63.0
FLOOR = 125 * 0.6931471805599453
TINY = 1e-30
CUTS = 2


def tile_rows(columns, most=24576):
    return 16 * max(1, most // (16 * columns))


def doubled(t):
    return jnp.concatenate([t, t], axis=0)


def limit(top):
    return (top * (1 + 2**-7)).astype(bf16)


def encode(t, scale):
    size = jnp.exp(POWER * jnp.log(1 + jnp.abs(t) * scale) - FLOOR)
    return jnp.where(t < 0, -size, size).astype(bf16)


def decode(t, scale):
    t = t.astype(f32)
    size = (jnp.exp((jnp.log(jnp.abs(t)) + FLOOR) * (1 / POWER)) - 1) * scale
    return jnp.where(t < 0, -size, size)


def coded_at(row, column, wide):
    return pl.ds(pl.multiple_of(row * wide + column * 16, 16), 16)


def settle(copies):
    for copy in copies:
        copy.wait_recv()


def kernel(
    replicas, models,
    g_ref, u_ref, d_ref, pg_ref, pu_ref, pd_ref, sn_ref, pn_ref,
    hg_ref, hu_ref, hd_ref, ng_ref, nu_ref, nd_ref, hn_ref, nn_ref,
    pr_g, pr_u, pr_d, pm_g, pm_u, pm_d, c1, r1, c2, r2, ow_w, ow_d,
    nrm_w, nrm_d, zs_w, zr_w, zs_d, zr_d, ratios, vs, vr, whole,
    ow_sem, pm_sem, pr_send, pr_recv, s1_send, s1_recv, s2_send, s2_recv,
    z_send, z_recv, v_send, v_recv, ag_send, ag_recv, ag_pair,
):
    me = lax.axis_index("replica")
    z = lax.axis_index("model")
    k = lax.rem(me, 2)
    x = lax.rem(me // 2, 2)
    y = me // 4
    partner = me + 1 - 2 * k
    xn = me + 2 - 4 * x
    yn = me + 4 - 8 * y
    rate = replicas ** (-0.5)

    slopes = (g_ref, u_ref, d_ref)
    halves = (hg_ref, hu_ref, hd_ref)
    mn = (ng_ref, nu_ref, nd_ref)
    pr = (pr_g, pr_u, pr_d)
    params = (pm_g, pm_u, pm_d)
    units = 2 * PIECES
    side = nd_ref.shape[1]
    bands = ng_ref.shape[0] // 128

    near, far = z + 1 - 2 * lax.rem(z, 2), z + 2 - 4 * (z // 2)
    barrier = pltpu.get_barrier_semaphore()
    around = [(partner, z), (xn, z), (yn, z), (me, near), (me, far)]
    for to in around:
        pl.semaphore_signal(barrier, inc=1, device_id=to, device_id_type=MESH)

    sequence = [h * PIECES + j for j in range(PIECES) for h in range(2)]
    jobs = [(m, u) for m in range(3) for u in sequence]
    steps = len(jobs) // 2

    def remote(src, dst, send_sem, recv_sem, to):
        return pltpu.make_async_remote_copy(
            src_ref=src, dst_ref=dst, send_sem=send_sem, recv_sem=recv_sem,
            device_id=to, device_id_type=MESH,
        )

    def height(m):
        return mn[m].shape[0] // units

    def parts(u):
        if u < PIECES:
            return [(1 - y, 1 - x), (y, 1 - x), (1 - y, x), (y, x)]
        return [(1 - y, 1 - x), (1 - y, x), (y, 1 - x), (y, x)]

    def view(m, u, q, core):
        rows = pl.ds(u * height(m), height(m))
        a, b = parts(u)[q]
        if m < 2:
            return slopes[m].at[a, b, core, rows, :]
        at = pl.multiple_of((2 * (2 * a + b) + core) * side, side)
        return slopes[m].at[rows, pl.ds(at, side)]

    def own_copy(n, q):
        m, u = jobs[n]
        ow = ow_w if m < 2 else ow_d
        return pltpu.make_async_copy(view(m, u, q, k), ow.at[n % SLOTS, q], ow_sem.at[n % SLOTS, q])

    def pair_copy(n, q):
        m, u = jobs[n]
        sem = 3 * n + min(q, 2) if n < units else 2 * units + n
        return remote(
            view(m, u, q, 1 - k), pr[m].at[u, q], pr_send.at[m], pr_recv.at[sem], (partner, z)
        )

    def await_pair(n, q):
        m, u = jobs[n]
        if n < units:
            at = pr[m].at[u, q] if q < 2 else pr[m].at[u, pl.ds(2, 2)]
            settle([remote(at, at, pr_send.at[m], pr_recv.at[3 * n + q], (partner, z))])
        elif q == 0:
            at = pr[m].at[u]
            settle([remote(at, at, pr_send.at[m], pr_recv.at[2 * units + n], (partner, z))])

    for n in range(SLOTS):
        for q in range(4):
            own_copy(n, q).start()
    loads = [
        pltpu.make_async_copy(src, params[m], pm_sem.at[m])
        for m, src in enumerate((pg_ref, pu_ref, pd_ref))
    ]

    tall, share = hn_ref.shape[0], nn_ref.shape[0]

    def vector_copy(step):
        to = (partner, xn, yn)[step]
        return remote(vs.at[step], vr.at[step], v_send.at[step], v_recv.at[step], (to, z))

    def send_vectors(step):
        if step == 0:
            line = lax.broadcasted_iota(jnp.int32, (tall, 128), 0)
            params_of_all = jnp.concatenate([pn_ref[...]] * replicas)
            vs[0, :tall] = sn_ref[...]
            vs[0, tall:] = jnp.where(line // share == me, params_of_all, 0)
        else:
            vs[step] = sum_vectors(step - 1)
        vector_copy(step).start()

    def sum_vectors(step):
        settle([vector_copy(step)])
        return vs[step] + vr[step]

    pl.semaphore_wait(barrier, len(around))

    send_vectors(0)

    for q in range(2):
        for n in range(2):
            pair_copy(n, q).start()
    for n in range(2):
        for q in range(2, 4):
            pair_copy(n, q).start()
    for n in range(2, len(jobs)):
        for q in range(4):
            pair_copy(n, q).start()
    for copy in loads:
        copy.start()

    def first_copy(n, p):
        m, u = jobs[n]
        return remote(
            c1.at[n % units, p], r1.at[m, u, p], s1_send.at[n % units, p],
            s1_recv.at[n] if p == 0 else s2_recv.at[n], (xn if u < PIECES else yn, z),
        )

    def second_copy(n):
        m, u = jobs[n]
        return remote(
            c2.at[n % units], r2.at[m, u], s2_send.at[n % units], s2_recv.at[n],
            (yn if u < PIECES else xn, z),
        )

    def await_rest(n):
        at = r1.at[jobs[n]]
        settle([remote(at, at, s2_send.at[n % units], s2_recv.at[n], (xn, z))])

    def sweep(m, body, carry=None):
        step = tile_rows(mn[m].shape[1])
        trips = height(m) // step
        if carry is None:
            pl.loop(0, trips)(lambda i: body(i * step, step))
            return None
        return lax.fori_loop(0, trips, lambda i, c: body(i * step, step, c), carry)

    def code_rows(m, read, dst):
        wide = mn[m].shape[1] // 128
        lane = lax.broadcasted_iota(jnp.int32, (16, 128), 1)

        def body(at, step, tops):
            values = read(at, step)
            for r in range(0, step, 16):
                line = [values[r : r + 16, c * 128 : (c + 1) * 128] for c in range(wide)]
                top = functools.reduce(jnp.maximum, [jnp.abs(t) for t in line])
                top = jnp.maximum(jnp.max(top, axis=1, keepdims=True), TINY)
                top = limit(jnp.broadcast_to(top, (16, 128))).astype(f32)
                scale = BEND / top
                for c, t in enumerate(line):
                    dst[coded_at(at + r, c, wide), :] = encode(t, scale)
                tops = jnp.where(lane == (at + r) // 16, top, tops)
            return tops

        tops = sweep(m, body, jnp.full((16, 128), TINY, f32))
        dst[dst.shape[0] - 16 :, :] = tops.astype(bf16)

    def code_columns(m, read, values, dst):
        wide = mn[m].shape[1] // 128

        def highest(at, step, tops):
            t = jnp.abs(read(at, step))
            for r in range(0, step, 8):
                tops = jnp.maximum(tops, t[r : r + 8])
            return tops

        tops = sweep(m, highest, jnp.full((8, wide * 128), TINY, f32))
        tops = limit(jnp.broadcast_to(jnp.max(tops, axis=0, keepdims=True), tops.shape))
        tops = tops.astype(f32)
        each = [tops[:, c * 128 : (c + 1) * 128] for c in range(wide)]
        scales = [doubled(BEND / top) for top in each]
        dst[dst.shape[0] - 16 :, :] = jnp.concatenate(each, axis=0).astype(bf16)

        def body(at, step):
            for r in range(0, step, 16):
                rows = pl.ds(pl.multiple_of(at + r, 16), 16)
                for c in range(wide):
                    t = values[rows, c * 128 : (c + 1) * 128]
                    dst[coded_at(at + r, c, wide), :] = encode(t, scales[c])

        sweep(m, body)

    def code_out(m, read, values, dst):
        if m < 2:
            code_rows(m, read, dst)
        else:
            code_columns(m, read, values, dst)

    def scales_of(m, src, at):
        tops = src[src.shape[0] - 16 :, :].astype(f32) * (1 / BEND)
        wide = mn[m].shape[1] // 128
        if m == 2:
            each = [doubled(tops[c * 8 : (c + 1) * 8]) for c in range(wide)]
            return lambda r: each
        lane = lax.broadcasted_iota(jnp.int32, (16, 128), 1)

        def of(r):
            top = jnp.where(lane == (at + r) // 16, tops, 0)
            return [jnp.broadcast_to(jnp.max(top, axis=1, keepdims=True), (16, 128))] * wide

        return of

    def decoded(m, src, at, step):
        wide = mn[m].shape[1] // 128
        of = scales_of(m, src, at)
        rows = []
        for r in range(0, step, 16):
            scales = of(r)
            line = [decode(src[coded_at(at + r, c, wide), :], scales[c]) for c in range(wide)]
            rows.append(jnp.concatenate(line, axis=1))
        return jnp.concatenate(rows, axis=0) if len(rows) > 1 else rows[0]

    def add(n, q, at, step):
        m, u = jobs[n]
        ow = ow_w if m < 2 else ow_d
        rows = pl.ds(pl.multiple_of(at, 16), step)
        both = pr[m][u, q, rows, :] + ow[n % SLOTS, q, rows, :]
        if m == 2 or q >= 2:
            pr[m][u, q, rows, :] = both
        return both

    def stage_1(n, p):
        m, u = jobs[n]
        own_copy(n, p).wait()
        await_pair(n, p)
        if n >= units:
            first_copy(n - units, p).wait_send()
        code_out(
            m, lambda at, step: add(n, p, at, step), pr[m].at[u, p], c1.at[n % units, p]
        )
        first_copy(n, p).start()

    def stage_1_rest(n):
        m, u = jobs[n]
        await_pair(n, 2)
        for q in range(2, 4):
            own_copy(n, q).wait()

            def keep(at, step):
                add(n, q, at, step)

            sweep(m, keep)
        if n + SLOTS < len(jobs):
            for q in range(4):
                own_copy(n + SLOTS, q).start()

    def stage_2(n):
        m, u = jobs[n]
        settle([first_copy(n, 0)])

        def both(at, step):
            rows = pl.ds(pl.multiple_of(at, 16), step)
            total = pr[m][u, 2, rows, :] + decoded(m, r1.at[m, u, 0], at, step)
            if m == 2:
                pr[m][u, 2, rows, :] = total
            return total

        if n >= units:
            second_copy(n - units).wait_send()
        code_out(m, both, pr[m].at[u, 2], c2.at[n % units])
        second_copy(n).start()

    def lanes(t):
        total = t[:, :128]
        for c in range(1, t.shape[1] // 128):
            total = total + t[:, c * 128 : (c + 1) * 128]
        return total

    def sublanes(t):
        total = t[:8]
        for c in range(1, t.shape[0] // 8):
            total = total + t[c * 8 : (c + 1) * 8]
        return total

    def stage_3(n):
        m, u = jobs[n]
        await_rest(n)
        if u == sequence[0]:
            loads[m].wait()
            if m == 2:
                nrm_d[...] = jnp.zeros_like(nrm_d)

        def body(at, step):
            rows = pl.ds(pl.multiple_of(at, 16), step)
            here = pl.ds(pl.multiple_of(u * height(m) + at, 16), step)
            mean = pr[m][u, 3, rows, :] + decoded(m, r1.at[m, u, 1], at, step)
            mean = (mean + decoded(m, r2.at[m, u], at, step)) * rate
            param = params[m][here, :]
            mn[m][here, :] = mean
            if m < 2:
                nrm_w[0, here, :] = lanes(param * param)
                nrm_w[1, here, :] = lanes(mean * mean)
            else:
                nrm_d[0] = nrm_d[0] + sublanes(param * param)
                nrm_d[1] = nrm_d[1] + sublanes(mean * mean)

        sweep(m, body)

    def sizes(m, step):
        out, back = (zs_w.at[m], zr_w.at[m]) if m < 2 else (zs_d, zr_d)
        return out.at[step], back.at[step]

    def size_copy(m, step):
        out, back = sizes(m, step)
        to = (me, near if step == 0 else far)
        return remote(out, back, z_send.at[m, step], z_recv.at[m, step], to)

    def send_sizes(m):
        if m < 2:
            for q in range(2):
                for b in range(bands):
                    block = nrm_w[q, b * 128 : (b + 1) * 128, :]
                    row = q * bands + b
                    zs_w[m, 0, row : row + 1, :] = jnp.sum(block.T, axis=0, keepdims=True)
        else:
            zs_d[0] = nrm_d[...]
        size_copy(m, 0).start()

    def all_sizes(m, step):
        settle([size_copy(m, step)])
        out, back = sizes(m, step)
        return out[...] + back[...]

    def relay_sizes(m):
        both = all_sizes(m, 0)
        sizes(m, 1)[0][...] = both
        size_copy(m, 1).start()

    def piece(m, chip, core, h):
        ref = halves[m]
        tall = mn[m].shape[0] // 2
        if m < 2:
            at = pl.multiple_of((2 * chip + core) * mn[0].shape[0], mn[0].shape[0])
            return ref.at[pl.ds(pl.multiple_of(at + h * tall, tall), tall), :]
        at = pl.multiple_of((2 * chip + core) * side, side)
        return ref.at[pl.ds(h * tall, tall), pl.ds(at, side)]

    chip, chip_x, chip_y, chip_d = me // 2, xn // 2, yn // 2, 3 - me // 2

    def gather(m, h, way, at, to):
        sem = ag_recv.at[m, h, way] if way < 3 else ag_pair.at[m]
        return remote(at, at, ag_send.at[m], sem, (to, z))

    def gathered(m, count):
        rows, columns = mn[m].shape
        if m < 2:
            at = halves[m].at[pl.ds(0, rows * count // 2), :]
        else:
            at = halves[m].at[:, pl.ds(0, columns * count // 2)]
        return remote(at, at, ag_send.at[m], ag_pair.at[m], (partner, z))

    def await_piece(m, h, way, chip_from, core):
        at = piece(m, chip_from, core, h)
        settle([gather(m, h, way, at, partner)])
        return at

    def update(m):
        total = all_sizes(m, 1)
        if m == 2:
            own = jnp.sum(total[0], axis=0, keepdims=True)
            size = jnp.sum(total[1], axis=0, keepdims=True)
            ratio_d = jnp.sqrt(own) * lax.rsqrt(size + eps)
        else:
            ratio = jnp.sqrt(total[:bands]) * lax.rsqrt(total[bands : 2 * bands] + eps)
            for b in range(bands):
                ratios[b * 128 : (b + 1) * 128, :] = jnp.broadcast_to(
                    ratio[b : b + 1], (128, 128)
                ).T
        columns = mn[m].shape[1]
        step = tile_rows(columns)
        tall = mn[m].shape[0] // 2
        for h in range(2):
            at = piece(m, chip, k, h)

            @pl.loop(0, tall // step)
            def _(i):
                here = pl.ds(pl.multiple_of(i * step, 16), step)
                rows = pl.ds(pl.multiple_of(h * tall + i * step, 16), step)
                if m < 2:
                    ratio = jnp.concatenate([ratios[rows, :]] * (columns // 128), axis=1)
                else:
                    ratio = ratio_d
                new = params[m][rows, :] - learn_rate * (mn[m][rows, :] * ratio)
                mn[m][rows, :] = new
                at[here, :] = new.astype(bf16)

            for way, to in ((0, xn), (1, yn), (3, partner)):
                gather(m, h, way, at, to).start()

    def relay(m, h, way, chip_from, *targets):
        at = await_piece(m, h, way, chip_from, k)
        for to_way, to in targets:
            gather(m, h, to_way, at, to).start()

    def forward(m):
        relay(m, 0, 0, chip_x, (2, yn), (3, partner))
        relay(m, 1, 1, chip_y, (2, xn), (3, partner))

    def hand_over(m):
        relay(m, 1, 0, chip_x, (3, partner))
        relay(m, 0, 1, chip_y, (3, partner))
        for h in range(2):
            relay(m, h, 2, chip_d, (3, partner))

    def finish_vectors():
        total = sum_vectors(2)
        whole[...] = total[tall:] - learn_rate * (total[:tall] * rate)
        hn_ref[...] = whole[...].astype(bf16)
        nn_ref[...] = whole[pl.ds(me * share, share), :]

    for t in range(steps + 2):
        if t < steps:
            for p in range(2):
                for n in (2 * t, 2 * t + 1):
                    stage_1(n, p)
            for n in (2 * t, 2 * t + 1):
                stage_1_rest(n)
        due, rest = divmod(t - 2, PIECES)
        updates = t > 2 and rest == 0 and 1 <= due <= 2
        if 0 <= t - 1 < steps:
            stage_2(2 * t - 2)
            stage_2(2 * t - 1)
        if updates:
            relay_sizes(due - 1)
        if 0 <= t - 2 < steps:
            stage_3(2 * t - 4)
            stage_3(2 * t - 3)
        done, rest = divmod(t - 2 + 1, PIECES)
        if t >= 2 and rest == 0 and done >= 1:
            send_sizes(done - 1)
        if updates:
            update(due - 1)
        if t in (2, 5):
            send_vectors(t // 2)
    forward(0)
    relay_sizes(2)
    update(2)
    finish_vectors()
    forward(1)
    forward(2)
    for m in range(3):
        hand_over(m)
    for m in range(3):
        settle([gathered(m, replicas)])
    for n in range(len(jobs) - units, len(jobs)):
        for p in range(2):
            first_copy(n, p).wait_send()
        second_copy(n).wait_send()
    for m in range(3):
        remote(pr[m], pr[m], pr_send.at[m], pr_recv.at[0], (partner, z)).wait_send()
        for step in range(2):
            size_copy(m, step).wait_send()
        gathered(m, 2 * replicas - 2).wait_send()
    for step in range(3):
        vector_copy(step).wait_send()


def put(*refs):
    count = len(refs) // 2
    copies = []
    for n, (src, dst) in enumerate(zip(refs[:count], refs[count : 2 * count])):
        rows = src.shape[0]
        tall = rows // CUTS if rows % (32 * CUTS) == 0 else rows
        for c in range(rows // tall):
            at = pl.ds(c * tall, tall)
            copies.append(pltpu.make_async_copy(src.at[at], dst.at[at], refs[-1].at[n, c]))
    for copy in copies:
        copy.start()
    for copy in copies:
        copy.wait()


def fused(replicas, models):
    def run(
        slope_gate, slope_up, slope_down, slope_norm, param_gate, param_up, param_down, param_norm
    ):
        rows, columns = param_gate.shape
        tall, side = param_down.shape
        units = 2 * PIECES
        tall_n, share = slope_norm.shape[1] // 128, param_norm.shape[0] // 128
        wide, deep = (rows // units, columns), (tall // units, side)
        coded = (rows // units * columns // 128 + 16, 128)
        V, DMA = pltpu.VMEM, pltpu.SemaphoreType.DMA
        by_chip = (2, replicas // 4, 2, rows, columns)
        whole, inside = pl.BlockSpec(memory_space=pl.ANY), pl.BlockSpec(memory_space=pltpu.VMEM)

        def three(front, dtype):
            return [V(front + wide, dtype), V(front + wide, dtype), V(front + deep, dtype)]

        out = pl.pallas_call(
            functools.partial(kernel, replicas, models),
            out_shape=(
                V((rows * replicas, columns), bf16),
                V((rows * replicas, columns), bf16),
                V((tall, side * replicas), bf16),
                V((rows, columns), f32),
                V((rows, columns), f32),
                V((tall, side), f32),
                V((tall_n, 128), bf16),
                V((share, 128), f32),
            ),
            in_specs=[whole] * 6 + [inside] * 2,
            out_specs=tuple([inside] * 8),
            scratch_shapes=[
                *three((units, 4), f32),
                V((rows, columns), f32), V((rows, columns), f32), V((tall, side), f32),
                V((units, 2) + coded, bf16), V((3, units, 2) + coded, bf16),
                V((units,) + coded, bf16), V((3, units) + coded, bf16),
                V((SLOTS, 4) + wide, f32), V((SLOTS, 4) + deep, f32),
                V((2, rows, 128), f32), V((2, 8, side), f32),
                V((2, 2, 2 * rows // 128, 128), f32), V((2, 2, 2 * rows // 128, 128), f32),
                V((2, 2, 8, side), f32), V((2, 2, 8, side), f32), V((rows, 128), f32),
                V((3, 2 * tall_n, 128), f32), V((3, 2 * tall_n, 128), f32), V((tall_n, 128), f32),
                DMA((SLOTS, 4)), DMA((3,)), DMA((3,)), DMA((5 * units,)),
                DMA((units, 2)), DMA((3 * units,)), DMA((units,)), DMA((3 * units,)),
                DMA((3, 2)), DMA((3, 2)), DMA((3,)), DMA((3,)),
                DMA((3,)), DMA((3, 2, 3)), DMA((3,)),
            ],
            compiler_params=pltpu.CompilerParams(
                collective_id=0, has_side_effects=True, vmem_limit_bytes=KERNEL_BYTES
            ),
        )(
            slope_gate.reshape(by_chip), slope_up.reshape(by_chip), slope_down[0],
            param_gate, param_up, param_down,
            slope_norm.reshape(tall_n, 128), param_norm.reshape(share, 128),
        )
        half_gate, half_up, half_down, next_gate, next_up, next_down, half_norm, next_norm = (
            pl.pallas_call(
                put,
                out_shape=tuple(jax.ShapeDtypeStruct(o.shape, o.dtype) for o in out),
                in_specs=[inside] * len(out),
                out_specs=tuple([whole] * len(out)),
                scratch_shapes=[DMA((len(out), CUTS))],
                compiler_params=pltpu.CompilerParams(vmem_limit_bytes=1 << 20),
            )(*[pltpu.with_memory_space_constraint(o, pltpu.VMEM) for o in out])
        )
        return (
            half_gate, half_up, half_down, half_norm.reshape(-1),
            next_gate, next_up, next_down, next_norm.reshape(-1),
        )

    return run


def plain(
    slope_gate, slope_up, slope_down, slope_norm, param_gate, param_up, param_down, param_norm
):
    rate = lax.axis_size("replica") ** (-0.5)
    halves, nexts = [], []
    for slope, param, dim in (
        (slope_gate, param_gate, 0), (slope_up, param_up, 0), (slope_down, param_down, 1)
    ):
        mean = lax.psum_scatter(slope[0], "replica", scatter_dimension=dim, tiled=True) * rate
        own, size = lax.psum(
            (
                jnp.sum(param * param, axis=1 - dim, keepdims=True),
                jnp.sum(mean * mean, axis=1 - dim, keepdims=True),
            ),
            "model",
        )
        new = param - learn_rate * (mean * (jnp.sqrt(own) * lax.rsqrt(size + eps)))
        nexts.append(new)
        halves.append(lax.all_gather(new.astype(bf16), "replica", axis=dim, tiled=True))
    mean = lax.psum_scatter(slope_norm[0], "replica", scatter_dimension=0, tiled=True) * rate
    new = param_norm - learn_rate * mean
    nexts.append(new)
    halves.append(lax.all_gather(new.astype(bf16), "replica", axis=0, tiled=True))
    return (*halves, *nexts)


def solution(mesh):
    replicas, models = mesh.shape["replica"], mesh.shape["model"]
    body = fused(replicas, models) if replicas == 2 * 2 * 2 and models == 4 else plain
    matrix, turned = P("replica", "model"), P("model", "replica")
    return jax.shard_map(
        body,
        mesh=mesh,
        in_specs=(
            P("replica", None, "model"),
            P("replica", None, "model"),
            P("replica", "model", None),
            P("replica", None),
            matrix, matrix, turned, P("replica"),
        ),
        out_specs=(
            P(None, "model"), P(None, "model"), P("model", None), P(),
            matrix, matrix, turned, P("replica"),
        ),
        check_vma=False,
    )
```

```python
import functools

import jax
import jax.numpy as jnp
from jax import lax
from jax.experimental import pallas as pl
from jax.experimental.pallas import tpu as pltpu
from jax.sharding import PartitionSpec as P

learn_rate = 0.5
eps = 1e-06
MESH = pl.DeviceIdType.MESH
f32, bf16 = jnp.float32, jnp.bfloat16
PIECES = 2
SLOTS = 2
KERNEL_BYTES = 43000000
BEND = 15.0
POWER = 63.0
FLOOR = 125 * 0.6931471805599453
TINY = 1e-30
CUTS = 2


def tile_rows(columns, most=24576):
    return 16 * max(1, most // (16 * columns))


def doubled(t):
    return jnp.concatenate([t, t], axis=0)


def limit(top):
    return (top * (1 + 2**-7)).astype(bf16)


def encode(t, scale):
    size = jnp.exp(POWER * jnp.log(1 + jnp.abs(t) * scale) - FLOOR)
    return jnp.where(t < 0, -size, size).astype(bf16)


def decode(t, scale):
    t = t.astype(f32)
    size = (jnp.exp((jnp.log(jnp.abs(t)) + FLOOR) * (1 / POWER)) - 1) * scale
    return jnp.where(t < 0, -size, size)


def coded_at(row, column, wide):
    return pl.ds(pl.multiple_of(row * wide + column * 16, 16), 16)


def settle(copies):
    for copy in copies:
        copy.wait_recv()


def kernel(
    replicas, models,
    g_ref, u_ref, d_ref, pg_ref, pu_ref, pd_ref, sn_ref, pn_ref,
    hg_ref, hu_ref, hd_ref, ng_ref, nu_ref, nd_ref, hn_ref, nn_ref,
    pr_g, pr_u, pr_d, pm_g, pm_u, pm_d, c1, r1, c2, r2, ow_w, ow_d,
    nrm_w, nrm_d, zs_w, zr_w, zs_d, zr_d, ratios, vs, vr, whole,
    st_sem, ow_sem, pm_sem, pr_send, pr_recv, s1_send, s1_recv, s2_send, s2_recv,
    z_send, z_recv, v_send, v_recv, ag_send, ag_recv, ag_pair,
):
    me = lax.axis_index("replica")
    z = lax.axis_index("model")
    k = lax.rem(me, 2)
    x = lax.rem(me // 2, 2)
    y = me // 4
    partner = me + 1 - 2 * k
    xn = me + 2 - 4 * x
    yn = me + 4 - 8 * y
    rate = replicas ** (-0.5)

    slopes = (g_ref, u_ref, d_ref)
    halves = (hg_ref, hu_ref, hd_ref)
    mn = (ng_ref, nu_ref, nd_ref)
    pr = (pr_g, pr_u, pr_d)
    params = (pm_g, pm_u, pm_d)
    units = 2 * PIECES
    side = nd_ref.shape[1]
    bands = ng_ref.shape[0] // 128

    near, far = z + 1 - 2 * lax.rem(z, 2), z + 2 - 4 * (z // 2)
    barrier = pltpu.get_barrier_semaphore()
    around = [(partner, z), (xn, z), (yn, z), (me, near), (me, far)]
    for to in around:
        pl.semaphore_signal(barrier, inc=1, device_id=to, device_id_type=MESH)

    sequence = [h * PIECES + j for j in range(PIECES) for h in range(2)]
    jobs = [(m, u) for m in range(3) for u in sequence]
    steps = len(jobs) // 2

    def remote(src, dst, send_sem, recv_sem, to):
        return pltpu.make_async_remote_copy(
            src_ref=src, dst_ref=dst, send_sem=send_sem, recv_sem=recv_sem,
            device_id=to, device_id_type=MESH,
        )

    def height(m):
        return mn[m].shape[0] // units

    def parts(u):
        if u < PIECES:
            return [(1 - y, 1 - x), (y, 1 - x), (1 - y, x), (y, x)]
        return [(1 - y, 1 - x), (1 - y, x), (y, 1 - x), (y, x)]

    def view(m, u, q, core):
        rows = pl.ds(u * height(m), height(m))
        a, b = parts(u)[q]
        if m < 2:
            return slopes[m].at[a, b, core, rows, :]
        at = pl.multiple_of((2 * (2 * a + b) + core) * side, side)
        return slopes[m].at[rows, pl.ds(at, side)]

    def own_copy(n, q):
        m, u = jobs[n]
        ow = ow_w if m < 2 else ow_d
        return pltpu.make_async_copy(view(m, u, q, k), ow.at[n % SLOTS, q], ow_sem.at[n % SLOTS, q])

    def pair_copy(n, q):
        m, u = jobs[n]
        sem = 3 * n + min(q, 2) if n < units else 2 * units + n
        return remote(
            view(m, u, q, 1 - k), pr[m].at[u, q], pr_send.at[m], pr_recv.at[sem], (partner, z)
        )

    def await_pair(n, q):
        m, u = jobs[n]
        if n < units:
            at = pr[m].at[u, q] if q < 2 else pr[m].at[u, pl.ds(2, 2)]
            settle([remote(at, at, pr_send.at[m], pr_recv.at[3 * n + q], (partner, z))])
        elif q == 0:
            at = pr[m].at[u]
            settle([remote(at, at, pr_send.at[m], pr_recv.at[2 * units + n], (partner, z))])

    def staged(i):
        n, q = i % 2, i // 2
        m, u = jobs[n]
        at = mn[m].at[pl.ds(i * height(m), height(m)), :]
        here = pltpu.make_async_copy(view(m, u, q, 1 - k), at, st_sem.at[i])
        there = remote(
            at, pr[m].at[u, q], pr_send.at[3], pr_recv.at[3 * n + q], (partner, z)
        )
        return here, there

    for i in range(4):
        staged(i)[0].start()
    for n in range(SLOTS):
        for q in range(4):
            own_copy(n, q).start()
    loads = [
        pltpu.make_async_copy(src, params[m], pm_sem.at[m])
        for m, src in enumerate((pg_ref, pu_ref, pd_ref))
    ]

    tall, share = hn_ref.shape[0], nn_ref.shape[0]

    def vector_copy(step):
        to = (partner, xn, yn)[step]
        return remote(vs.at[step], vr.at[step], v_send.at[step], v_recv.at[step], (to, z))

    def send_vectors(step):
        if step == 0:
            line = lax.broadcasted_iota(jnp.int32, (tall, 128), 0)
            params_of_all = jnp.concatenate([pn_ref[...]] * replicas)
            vs[0, :tall] = sn_ref[...]
            vs[0, tall:] = jnp.where(line // share == me, params_of_all, 0)
        else:
            vs[step] = sum_vectors(step - 1)
        vector_copy(step).start()

    def sum_vectors(step):
        settle([vector_copy(step)])
        return vs[step] + vr[step]

    pl.semaphore_wait(barrier, len(around))

    send_vectors(0)

    for i in range(4):
        here, there = staged(i)
        here.wait()
        there.start()
    for n in range(2):
        for q in range(2, 4):
            pair_copy(n, q).start()
    for n in range(2, len(jobs)):
        for q in range(4):
            pair_copy(n, q).start()
    for copy in loads:
        copy.start()

    def first_copy(n, p):
        m, u = jobs[n]
        return remote(
            c1.at[n % units, p], r1.at[m, u, p], s1_send.at[n % units, p],
            s1_recv.at[n] if p == 0 else s2_recv.at[n], (xn if u < PIECES else yn, z),
        )

    def second_copy(n):
        m, u = jobs[n]
        return remote(
            c2.at[n % units], r2.at[m, u], s2_send.at[n % units], s2_recv.at[n],
            (yn if u < PIECES else xn, z),
        )

    def await_rest(n):
        at = r1.at[jobs[n]]
        settle([remote(at, at, s2_send.at[n % units], s2_recv.at[n], (xn, z))])

    def sweep(m, body, carry=None):
        step = tile_rows(mn[m].shape[1])
        trips = height(m) // step
        if carry is None:
            pl.loop(0, trips)(lambda i: body(i * step, step))
            return None
        return lax.fori_loop(0, trips, lambda i, c: body(i * step, step, c), carry)

    def code_rows(m, read, dst):
        wide = mn[m].shape[1] // 128
        lane = lax.broadcasted_iota(jnp.int32, (16, 128), 1)

        def body(at, step, tops):
            values = read(at, step)
            for r in range(0, step, 16):
                line = [values[r : r + 16, c * 128 : (c + 1) * 128] for c in range(wide)]
                top = functools.reduce(jnp.maximum, [jnp.abs(t) for t in line])
                top = jnp.maximum(jnp.max(top, axis=1, keepdims=True), TINY)
                top = limit(jnp.broadcast_to(top, (16, 128))).astype(f32)
                scale = BEND / top
                for c, t in enumerate(line):
                    dst[coded_at(at + r, c, wide), :] = encode(t, scale)
                tops = jnp.where(lane == (at + r) // 16, top, tops)
            return tops

        tops = sweep(m, body, jnp.full((16, 128), TINY, f32))
        dst[dst.shape[0] - 16 :, :] = tops.astype(bf16)

    def code_columns(m, read, values, dst):
        wide = mn[m].shape[1] // 128

        def highest(at, step, tops):
            t = jnp.abs(read(at, step))
            for r in range(0, step, 8):
                tops = jnp.maximum(tops, t[r : r + 8])
            return tops

        tops = sweep(m, highest, jnp.full((8, wide * 128), TINY, f32))
        tops = limit(jnp.broadcast_to(jnp.max(tops, axis=0, keepdims=True), tops.shape))
        tops = tops.astype(f32)
        each = [tops[:, c * 128 : (c + 1) * 128] for c in range(wide)]
        scales = [doubled(BEND / top) for top in each]
        dst[dst.shape[0] - 16 :, :] = jnp.concatenate(each, axis=0).astype(bf16)

        def body(at, step):
            for r in range(0, step, 16):
                rows = pl.ds(pl.multiple_of(at + r, 16), 16)
                for c in range(wide):
                    t = values[rows, c * 128 : (c + 1) * 128]
                    dst[coded_at(at + r, c, wide), :] = encode(t, scales[c])

        sweep(m, body)

    def code_out(m, read, values, dst):
        if m < 2:
            code_rows(m, read, dst)
        else:
            code_columns(m, read, values, dst)

    def scales_of(m, src, at):
        tops = src[src.shape[0] - 16 :, :].astype(f32) * (1 / BEND)
        wide = mn[m].shape[1] // 128
        if m == 2:
            each = [doubled(tops[c * 8 : (c + 1) * 8]) for c in range(wide)]
            return lambda r: each
        lane = lax.broadcasted_iota(jnp.int32, (16, 128), 1)

        def of(r):
            top = jnp.where(lane == (at + r) // 16, tops, 0)
            return [jnp.broadcast_to(jnp.max(top, axis=1, keepdims=True), (16, 128))] * wide

        return of

    def decoded(m, src, at, step):
        wide = mn[m].shape[1] // 128
        of = scales_of(m, src, at)
        rows = []
        for r in range(0, step, 16):
            scales = of(r)
            line = [decode(src[coded_at(at + r, c, wide), :], scales[c]) for c in range(wide)]
            rows.append(jnp.concatenate(line, axis=1))
        return jnp.concatenate(rows, axis=0) if len(rows) > 1 else rows[0]

    def add(n, q, at, step):
        m, u = jobs[n]
        ow = ow_w if m < 2 else ow_d
        rows = pl.ds(pl.multiple_of(at, 16), step)
        both = pr[m][u, q, rows, :] + ow[n % SLOTS, q, rows, :]
        if m == 2 or q >= 2:
            pr[m][u, q, rows, :] = both
        return both

    def stage_1(n, p):
        m, u = jobs[n]
        own_copy(n, p).wait()
        await_pair(n, p)
        if n >= units:
            first_copy(n - units, p).wait_send()
        code_out(
            m, lambda at, step: add(n, p, at, step), pr[m].at[u, p], c1.at[n % units, p]
        )
        first_copy(n, p).start()

    def stage_1_rest(n):
        m, u = jobs[n]
        await_pair(n, 2)
        for q in range(2, 4):
            own_copy(n, q).wait()

            def keep(at, step):
                add(n, q, at, step)

            sweep(m, keep)
        if n + SLOTS < len(jobs):
            for q in range(4):
                own_copy(n + SLOTS, q).start()

    def stage_2(n):
        m, u = jobs[n]
        settle([first_copy(n, 0)])

        def both(at, step):
            rows = pl.ds(pl.multiple_of(at, 16), step)
            total = pr[m][u, 2, rows, :] + decoded(m, r1.at[m, u, 0], at, step)
            if m == 2:
                pr[m][u, 2, rows, :] = total
            return total

        if n >= units:
            second_copy(n - units).wait_send()
        code_out(m, both, pr[m].at[u, 2], c2.at[n % units])
        second_copy(n).start()

    def lanes(t):
        total = t[:, :128]
        for c in range(1, t.shape[1] // 128):
            total = total + t[:, c * 128 : (c + 1) * 128]
        return total

    def sublanes(t):
        total = t[:8]
        for c in range(1, t.shape[0] // 8):
            total = total + t[c * 8 : (c + 1) * 8]
        return total

    def stage_3(n):
        m, u = jobs[n]
        await_rest(n)
        if u == sequence[0]:
            loads[m].wait()
            if m == 0:
                remote(mn[0], mn[0], pr_send.at[3], pr_recv.at[0], (partner, z)).wait_send()
            if m == 2:
                nrm_d[...] = jnp.zeros_like(nrm_d)

        def body(at, step):
            rows = pl.ds(pl.multiple_of(at, 16), step)
            here = pl.ds(pl.multiple_of(u * height(m) + at, 16), step)
            mean = pr[m][u, 3, rows, :] + decoded(m, r1.at[m, u, 1], at, step)
            mean = (mean + decoded(m, r2.at[m, u], at, step)) * rate
            param = params[m][here, :]
            mn[m][here, :] = mean
            if m < 2:
                nrm_w[0, here, :] = lanes(param * param)
                nrm_w[1, here, :] = lanes(mean * mean)
            else:
                nrm_d[0] = nrm_d[0] + sublanes(param * param)
                nrm_d[1] = nrm_d[1] + sublanes(mean * mean)

        sweep(m, body)

    def sizes(m, step):
        out, back = (zs_w.at[m], zr_w.at[m]) if m < 2 else (zs_d, zr_d)
        return out.at[step], back.at[step]

    def size_copy(m, step):
        out, back = sizes(m, step)
        to = (me, near if step == 0 else far)
        return remote(out, back, z_send.at[m, step], z_recv.at[m, step], to)

    def send_sizes(m):
        if m < 2:
            for q in range(2):
                for b in range(bands):
                    block = nrm_w[q, b * 128 : (b + 1) * 128, :]
                    row = q * bands + b
                    zs_w[m, 0, row : row + 1, :] = jnp.sum(block.T, axis=0, keepdims=True)
        else:
            zs_d[0] = nrm_d[...]
        size_copy(m, 0).start()

    def all_sizes(m, step):
        settle([size_copy(m, step)])
        out, back = sizes(m, step)
        return out[...] + back[...]

    def relay_sizes(m):
        both = all_sizes(m, 0)
        sizes(m, 1)[0][...] = both
        size_copy(m, 1).start()

    def piece(m, chip, core, h):
        ref = halves[m]
        tall = mn[m].shape[0] // 2
        if m < 2:
            at = pl.multiple_of((2 * chip + core) * mn[0].shape[0], mn[0].shape[0])
            return ref.at[pl.ds(pl.multiple_of(at + h * tall, tall), tall), :]
        at = pl.multiple_of((2 * chip + core) * side, side)
        return ref.at[pl.ds(h * tall, tall), pl.ds(at, side)]

    chip, chip_x, chip_y, chip_d = me // 2, xn // 2, yn // 2, 3 - me // 2

    def gather(m, h, way, at, to):
        sem = ag_recv.at[m, h, way] if way < 3 else ag_pair.at[m]
        return remote(at, at, ag_send.at[m], sem, (to, z))

    def gathered(m, count):
        rows, columns = mn[m].shape
        if m < 2:
            at = halves[m].at[pl.ds(0, rows * count // 2), :]
        else:
            at = halves[m].at[:, pl.ds(0, columns * count // 2)]
        return remote(at, at, ag_send.at[m], ag_pair.at[m], (partner, z))

    def await_piece(m, h, way, chip_from, core):
        at = piece(m, chip_from, core, h)
        settle([gather(m, h, way, at, partner)])
        return at

    def update(m):
        total = all_sizes(m, 1)
        if m == 2:
            own = jnp.sum(total[0], axis=0, keepdims=True)
            size = jnp.sum(total[1], axis=0, keepdims=True)
            ratio_d = jnp.sqrt(own) * lax.rsqrt(size + eps)
        else:
            ratio = jnp.sqrt(total[:bands]) * lax.rsqrt(total[bands : 2 * bands] + eps)
            for b in range(bands):
                ratios[b * 128 : (b + 1) * 128, :] = jnp.broadcast_to(
                    ratio[b : b + 1], (128, 128)
                ).T
        columns = mn[m].shape[1]
        step = tile_rows(columns)
        tall = mn[m].shape[0] // 2
        for h in range(2):
            at = piece(m, chip, k, h)

            @pl.loop(0, tall // step)
            def _(i):
                here = pl.ds(pl.multiple_of(i * step, 16), step)
                rows = pl.ds(pl.multiple_of(h * tall + i * step, 16), step)
                if m < 2:
                    ratio = jnp.concatenate([ratios[rows, :]] * (columns // 128), axis=1)
                else:
                    ratio = ratio_d
                new = params[m][rows, :] - learn_rate * (mn[m][rows, :] * ratio)
                mn[m][rows, :] = new
                at[here, :] = new.astype(bf16)

            for way, to in ((0, xn), (1, yn), (3, partner)):
                gather(m, h, way, at, to).start()

    def relay(m, h, way, chip_from, *targets):
        at = await_piece(m, h, way, chip_from, k)
        for to_way, to in targets:
            gather(m, h, to_way, at, to).start()

    def forward(m):
        relay(m, 0, 0, chip_x, (2, yn), (3, partner))
        relay(m, 1, 1, chip_y, (2, xn), (3, partner))

    def hand_over(m):
        relay(m, 1, 0, chip_x, (3, partner))
        relay(m, 0, 1, chip_y, (3, partner))
        for h in range(2):
            relay(m, h, 2, chip_d, (3, partner))

    def finish_vectors():
        total = sum_vectors(2)
        whole[...] = total[tall:] - learn_rate * (total[:tall] * rate)
        hn_ref[...] = whole[...].astype(bf16)
        nn_ref[...] = whole[pl.ds(me * share, share), :]

    for t in range(steps + 2):
        if t < steps:
            for p in range(2):
                for n in (2 * t, 2 * t + 1):
                    stage_1(n, p)
            for n in (2 * t, 2 * t + 1):
                stage_1_rest(n)
        due, rest = divmod(t - 2, PIECES)
        updates = t > 2 and rest == 0 and 1 <= due <= 2
        if 0 <= t - 1 < steps:
            stage_2(2 * t - 2)
            stage_2(2 * t - 1)
        if updates:
            relay_sizes(due - 1)
        if 0 <= t - 2 < steps:
            stage_3(2 * t - 4)
            stage_3(2 * t - 3)
        done, rest = divmod(t - 2 + 1, PIECES)
        if t >= 2 and rest == 0 and done >= 1:
            send_sizes(done - 1)
        if updates:
            update(due - 1)
        if t in (2, 5):
            send_vectors(t // 2)
    forward(0)
    relay_sizes(2)
    update(2)
    finish_vectors()
    forward(1)
    forward(2)
    for m in range(3):
        hand_over(m)
    for m in range(3):
        settle([gathered(m, replicas)])
    for n in range(len(jobs) - units, len(jobs)):
        for p in range(2):
            first_copy(n, p).wait_send()
        second_copy(n).wait_send()
    for m in range(3):
        at = pr[m].at[pl.ds(0, units - 1)] if m == 0 else pr[m]
        remote(at, at, pr_send.at[m], pr_recv.at[0], (partner, z)).wait_send()
        for step in range(2):
            size_copy(m, step).wait_send()
        gathered(m, 2 * replicas - 2).wait_send()
    for step in range(3):
        vector_copy(step).wait_send()


def put(*refs):
    count = len(refs) // 2
    copies = []
    for n, (src, dst) in enumerate(zip(refs[:count], refs[count : 2 * count])):
        rows = src.shape[0]
        tall = rows // CUTS if rows % (32 * CUTS) == 0 else rows
        for c in range(rows // tall):
            at = pl.ds(c * tall, tall)
            copies.append(pltpu.make_async_copy(src.at[at], dst.at[at], refs[-1].at[n, c]))
    for copy in copies:
        copy.start()
    for copy in copies:
        copy.wait()


def fused(replicas, models):
    def run(
        slope_gate, slope_up, slope_down, slope_norm, param_gate, param_up, param_down, param_norm
    ):
        rows, columns = param_gate.shape
        tall, side = param_down.shape
        units = 2 * PIECES
        tall_n, share = slope_norm.shape[1] // 128, param_norm.shape[0] // 128
        wide, deep = (rows // units, columns), (tall // units, side)
        coded = (rows // units * columns // 128 + 16, 128)
        V, DMA = pltpu.VMEM, pltpu.SemaphoreType.DMA
        by_chip = (2, replicas // 4, 2, rows, columns)
        whole, inside = pl.BlockSpec(memory_space=pl.ANY), pl.BlockSpec(memory_space=pltpu.VMEM)

        def three(front, dtype):
            return [V(front + wide, dtype), V(front + wide, dtype), V(front + deep, dtype)]

        out = pl.pallas_call(
            functools.partial(kernel, replicas, models),
            out_shape=(
                V((rows * replicas, columns), bf16),
                V((rows * replicas, columns), bf16),
                V((tall, side * replicas), bf16),
                V((rows, columns), f32),
                V((rows, columns), f32),
                V((tall, side), f32),
                V((tall_n, 128), bf16),
                V((share, 128), f32),
            ),
            in_specs=[whole] * 6 + [inside] * 2,
            out_specs=tuple([inside] * 8),
            scratch_shapes=[
                *three((units, 4), f32),
                V((rows, columns), f32), V((rows, columns), f32), V((tall, side), f32),
                V((units, 2) + coded, bf16), V((3, units, 2) + coded, bf16),
                V((units,) + coded, bf16), V((3, units) + coded, bf16),
                V((SLOTS, 4) + wide, f32), V((SLOTS, 4) + deep, f32),
                V((2, rows, 128), f32), V((2, 8, side), f32),
                V((2, 2, 2 * rows // 128, 128), f32), V((2, 2, 2 * rows // 128, 128), f32),
                V((2, 2, 8, side), f32), V((2, 2, 8, side), f32), V((rows, 128), f32),
                V((3, 2 * tall_n, 128), f32), V((3, 2 * tall_n, 128), f32), V((tall_n, 128), f32),
                DMA((4,)), DMA((SLOTS, 4)), DMA((3,)), DMA((4,)), DMA((5 * units,)),
                DMA((units, 2)), DMA((3 * units,)), DMA((units,)), DMA((3 * units,)),
                DMA((3, 2)), DMA((3, 2)), DMA((3,)), DMA((3,)),
                DMA((3,)), DMA((3, 2, 3)), DMA((3,)),
            ],
            compiler_params=pltpu.CompilerParams(
                collective_id=0, has_side_effects=True, vmem_limit_bytes=KERNEL_BYTES
            ),
        )(
            slope_gate.reshape(by_chip), slope_up.reshape(by_chip), slope_down[0],
            param_gate, param_up, param_down,
            slope_norm.reshape(tall_n, 128), param_norm.reshape(share, 128),
        )
        half_gate, half_up, half_down, next_gate, next_up, next_down, half_norm, next_norm = (
            pl.pallas_call(
                put,
                out_shape=tuple(jax.ShapeDtypeStruct(o.shape, o.dtype) for o in out),
                in_specs=[inside] * len(out),
                out_specs=tuple([whole] * len(out)),
                scratch_shapes=[DMA((len(out), CUTS))],
                compiler_params=pltpu.CompilerParams(vmem_limit_bytes=1 << 20),
            )(*[pltpu.with_memory_space_constraint(o, pltpu.VMEM) for o in out])
        )
        return (
            half_gate, half_up, half_down, half_norm.reshape(-1),
            next_gate, next_up, next_down, next_norm.reshape(-1),
        )

    return run


def plain(
    slope_gate, slope_up, slope_down, slope_norm, param_gate, param_up, param_down, param_norm
):
    rate = lax.axis_size("replica") ** (-0.5)
    halves, nexts = [], []
    for slope, param, dim in (
        (slope_gate, param_gate, 0), (slope_up, param_up, 0), (slope_down, param_down, 1)
    ):
        mean = lax.psum_scatter(slope[0], "replica", scatter_dimension=dim, tiled=True) * rate
        own, size = lax.psum(
            (
                jnp.sum(param * param, axis=1 - dim, keepdims=True),
                jnp.sum(mean * mean, axis=1 - dim, keepdims=True),
            ),
            "model",
        )
        new = param - learn_rate * (mean * (jnp.sqrt(own) * lax.rsqrt(size + eps)))
        nexts.append(new)
        halves.append(lax.all_gather(new.astype(bf16), "replica", axis=dim, tiled=True))
    mean = lax.psum_scatter(slope_norm[0], "replica", scatter_dimension=0, tiled=True) * rate
    new = param_norm - learn_rate * mean
    nexts.append(new)
    halves.append(lax.all_gather(new.astype(bf16), "replica", axis=0, tiled=True))
    return (*halves, *nexts)


def solution(mesh):
    replicas, models = mesh.shape["replica"], mesh.shape["model"]
    body = fused(replicas, models) if replicas == 2 * 2 * 2 and models == 4 else plain
    matrix, turned = P("replica", "model"), P("model", "replica")
    return jax.shard_map(
        body,
        mesh=mesh,
        in_specs=(
            P("replica", None, "model"),
            P("replica", None, "model"),
            P("replica", "model", None),
            P("replica", None),
            matrix, matrix, turned, P("replica"),
        ),
        out_specs=(
            P(None, "model"), P(None, "model"), P("model", None), P(),
            matrix, matrix, turned, P("replica"),
        ),
        check_vma=False,
    )
```
